32 devices in a mesh: freq: 2 (over x), panel: 16 (over z, y, core).
Axes of the slice: x: 2, y: 2, z: 4, core: 2. Of those that a mesh axis runs over, the one named last changes fastest.
Arguments:
- recorded: float32 [2, 2, 2048, 2048], P('freq', None, 'panel'), parts along dimension 0, may hold values from -60 to 60
- receiver_kernel: bfloat16 [2, 2, 4095], P('freq'), parts along dimension 0, may hold values from -1.5 to 1.5
- source_kernel: bfloat16 [2, 2, 4095], P('freq'), parts along dimension 0, may hold values from -1.5 to 1.5
Outputs:
- primaries: float32 [2, 2, 2048, 2048], P('freq', None, 'panel'), parts along dimension 0
- multiples: bfloat16 [2, 2, 2048, 2048], P('freq', None, 'panel'), parts along dimension 0
The draws below stay inside these ranges and needn't reach their ends.
There are 2 independent parts, one for each index of `freq`. The reference program is written for one: setup_inputs(seed, part) draws one part's arguments, and reference() takes and returns one part's arrays. A program takes and returns all parts, laid end to end along the dimension named above; each array names one. Nothing has to cross between parts.
All inputs are finite; a program needn't handle non-finite values.
Results may differ from the reference program's by a relative error of at most 0.0057.
Values may be sent and summed in bfloat16 or wider, within the bound.
A program may use at most 320 MiB of HBM per device.

```python
import math
import jax
import jax.numpy as jnp

FREQS = 1
NS = 2048
NR = 2048


def focal_kernel(key, width):
    key_taps, key_phase, key_mag = jax.random.split(key, 3)
    count = 2 * width - 1
    taps = jnp.clip(jax.random.normal(key_taps, (FREQS, 2, count), jnp.float32), -6.0, 6.0)
    taps = taps / jnp.sqrt(2.0 * width)
    phase = jax.random.uniform(key_phase, (FREQS, 1), jnp.float32, -math.pi, math.pi)
    magnitude = jax.random.uniform(key_mag, (FREQS, 1), jnp.float32, 0.8, 1.2)
    center = (jnp.arange(count) == width - 1)[None, :]
    real_part = jnp.where(center, magnitude * jnp.cos(phase), taps[:, 0])
    imag_part = jnp.where(center, magnitude * jnp.sin(phase), taps[:, 1])
    return jnp.stack([real_part, imag_part], axis=1).astype(jnp.bfloat16)


def draw_receiver_kernel(key, part):
    return focal_kernel(jax.random.fold_in(key, 11), NR)


def draw_source_kernel(key, part):
    return focal_kernel(jax.random.fold_in(key, 23), NS)


def draw_recorded(key, part):
    key_base, key_rows, key_cols = jax.random.split(jax.random.fold_in(key, 37), 3)
    rising = 3.0 ** (jnp.arange(NS, dtype=jnp.float32) / (NS - 1))
    base = jnp.clip(jax.random.normal(key_base, (FREQS, 2, NS, NR), jnp.float32), -6.0, 6.0)
    row_scale = jnp.exp(jax.random.uniform(key_rows, (NS,), jnp.float32, math.log(0.7), math.log(1.4)))
    col_scale = jnp.exp(jax.random.uniform(key_cols, (NR,), jnp.float32, math.log(0.7), math.log(1.4)))
    return base * (rising * row_scale)[:, None] * col_scale[None, :]


def setup_inputs(seed: int = 0, part: int = 0) -> dict:
    keys = jax.random.split(jax.random.key(seed), 4)
    part_splits = jax.random.split(jax.random.fold_in(keys[3], part), 4)
    return {
        "recorded": draw_recorded(jax.random.fold_in(jax.random.fold_in(keys[3], part), 71), part),
        "receiver_kernel": draw_receiver_kernel(jax.random.fold_in(jax.random.fold_in(keys[3], part), 71), part),
        "source_kernel": draw_source_kernel(jax.random.fold_in(jax.random.fold_in(keys[3], part), 71), part),
    }


def toeplitz(kernel, width):
    rows = jnp.arange(width, dtype=jnp.int32)[:, None]
    cols = jnp.arange(width, dtype=jnp.int32)[None, :]
    return kernel[:, cols - rows + width - 1]


def complex_dot(left, right):
    real_part = jnp.dot(left[0], right[0], preferred_element_type=jnp.float32) - jnp.dot(left[1], right[1], preferred_element_type=jnp.float32)
    imag_part = jnp.dot(left[0], right[1], preferred_element_type=jnp.float32) + jnp.dot(left[1], right[0], preferred_element_type=jnp.float32)
    return jnp.stack([real_part, imag_part])


def reference(recorded, receiver_kernel, source_kernel):
    prim_list = []
    mult_list = []
    for slot in range(FREQS):
        data = recorded[slot]
        data_b = data.astype(jnp.bfloat16)
        g_recv = toeplitz(receiver_kernel[slot], NR)
        g_src = toeplitz(source_kernel[slot], NS)
        focused = complex_dot(data_b, g_recv).astype(jnp.bfloat16)
        mult = complex_dot(g_src, focused).astype(jnp.bfloat16)
        mfl = mult.astype(jnp.float32)
        num_re = jnp.sum(mfl[0] * data[0] + mfl[1] * data[1])
        num_im = jnp.sum(mfl[0] * data[1] - mfl[1] * data[0])
        den = jnp.sum(mfl[0] * mfl[0] + mfl[1] * mfl[1]) + 1e-6
        fit_re = num_re / den
        fit_im = num_im / den
        prim_re = data[0] - (fit_re * mfl[0] - fit_im * mfl[1])
        prim_im = data[1] - (fit_re * mfl[1] + fit_im * mfl[0])
        prim_list.append(jnp.stack([prim_re, prim_im]))
        mult_list.append(mult)
    return jnp.stack(prim_list), jnp.stack(mult_list)
```

```python
import functools

import jax
import jax.numpy as jnp
from jax import lax
from jax.experimental import pallas as pl
from jax.experimental.pallas import tpu as pltpu
from jax.sharding import PartitionSpec as P

MESH = pl.DeviceIdType.MESH
LANES = 128
GROUP = 256
STRIP = 16
STRIPS = 4
PLANES = 4


def spread(taps_ref, padded, comp, flipped):
    length = padded.shape[1]
    rows = [padded[comp : comp + 1, at : at + LANES] for at in range(0, length, LANES)]
    if not flipped:
        return jnp.broadcast_to(jnp.concatenate(rows, axis=1), (STRIP, length))
    i = lax.broadcasted_iota(jnp.int32, (LANES, LANES), 0)
    j = lax.broadcasted_iota(jnp.int32, (LANES, LANES), 1)
    swap = jnp.where(i + j == LANES - 1, 1.0, 0.0).astype(jnp.bfloat16)
    tall = jnp.concatenate([jnp.broadcast_to(r, (STRIP, LANES)) for r in rows[::-1]], axis=0)
    tall = jnp.dot(tall.astype(jnp.bfloat16), swap, preferred_element_type=jnp.float32)
    return jnp.concatenate([tall[at : at + STRIP] for at in range(0, tall.shape[0], STRIP)], axis=1)


def skew(taps_ref, padded, flipped, block, band_ref):
    length = padded.shape[1]
    padded[...] = jnp.zeros_like(padded)
    padded[:, 0 : length - 1] = taps_ref[0].astype(jnp.float32)
    row = lax.broadcasted_iota(jnp.int32, (STRIP, length), 0)
    for comp in range(2):
        x = spread(taps_ref, padded, comp, flipped)
        step = 1
        while step < STRIP:
            x = jnp.where((row & step) != 0, pltpu.roll(x, step, 1), x)
            step *= 2
        lane0 = comp * block
        for s in range(0, LANES, STRIP):
            shift = (s - (LANES - block) + (0 if flipped else 1)) % length
            y = (pltpu.roll(x, shift, 1) if shift else x).astype(jnp.bfloat16)
            for m in range(length // LANES):
                at = length - LANES * (m + 1)
                band_ref[m * LANES + s : m * LANES + s + STRIP, lane0 : lane0 + block] = y[:, at : at + block]


def exchange_kernel(
    panels,
    rec_hbm,
    rtaps_hbm,
    staps_hbm,
    rec_ref,
    mult_ref,
    fit_ref,
    rtaps_ref,
    staps_ref,
    load_sem,
    padded,
    band_r,
    band_s,
    w1,
    w2,
    foc,
    foc_in,
    mul,
    mul_in,
    sums,
    sums_in,
    send1,
    recv1,
    send2,
    recv2,
    send3,
    recv3,
):
    me = lax.axis_index("panel")
    rows, width = rec_ref.shape[2], rec_ref.shape[3]
    sources = rows * panels
    cols = width // panels
    halves, hc = foc_in.shape[0], foc_in.shape[2]
    nt = (((1,), (1,)), ((), ()))
    planes = recv2.shape[0]
    side = panels // planes
    plane = me // side

    def order(n, own, groups):
        half = groups // 2
        far = lax.rem(own // half + 1 + n // half, 2)
        return far * half + lax.rem(own + 1 + n, half)

    def peer(o):
        return lax.rem(me + o, panels)

    loads = [
        pltpu.make_async_copy(src, dst, load_sem.at[i])
        for i, (src, dst) in enumerate(
            ((rtaps_hbm, rtaps_ref), (rec_hbm, rec_ref), (staps_hbm, staps_ref))
        )
    ]
    for load in loads:
        load.start()

    barrier = pltpu.get_barrier_semaphore()

    @pl.loop(1, panels)
    def _(o):
        pl.semaphore_signal(barrier, inc=1, device_id={"panel": peer(o)}, device_id_type=MESH)

    loads[0].wait()
    skew(rtaps_ref, padded, True, LANES, band_r)
    loads[1].wait()
    for kb in range(width // LANES):
        re = rec_ref[0, 0, :, kb * LANES : (kb + 1) * LANES].astype(jnp.bfloat16)
        im = rec_ref[0, 1, :, kb * LANES : (kb + 1) * LANES].astype(jnp.bfloat16)
        at = 2 * kb * LANES
        w1[0:rows, at : at + LANES] = re
        w1[0:rows, at + LANES : at + 2 * LANES] = -im
        w1[rows : 2 * rows, at : at + LANES] = im
        w1[rows : 2 * rows, at + LANES : at + 2 * LANES] = re

    pl.semaphore_wait(barrier, panels - 1)

    def copy1(h, dest, src):
        return pltpu.make_async_remote_copy(
            src_ref=foc.at[pl.ds(pl.multiple_of(dest * cols + h * hc, hc), hc), :],
            dst_ref=foc_in.at[h, src],
            send_sem=send1,
            recv_sem=recv1.at[h],
            device_id={"panel": dest},
            device_id_type=MESH,
        )

    def copy2(h, dest, src):
        return pltpu.make_async_remote_copy(
            src_ref=mul.at[h, pl.ds(pl.multiple_of(dest * rows, rows), rows), :],
            dst_ref=mul_in.at[h, src],
            send_sem=send2,
            recv_sem=recv2.at[src // side],
            device_id={"panel": dest},
            device_id_type=MESH,
        )

    def drain(ref, sem):
        pltpu.make_async_copy(ref, ref, sem).wait()

    def copy3(dest, src):
        return pltpu.make_async_remote_copy(
            src_ref=sums,
            dst_ref=sums_in.at[src],
            send_sem=send3,
            recv_sem=recv3,
            device_id={"panel": dest},
            device_id_type=MESH,
        )

    groups1 = width // GROUP
    per1 = GROUP // cols
    own1 = me // per1

    @pl.loop(0, groups1)
    def _(n):
        g = order(n, own1, groups1)
        first = pl.multiple_of(g * GROUP, GROUP)
        lhs = jnp.concatenate(
            [
                band_r[pl.ds(pl.multiple_of(width - LANES * (kb + 1) + first, LANES), GROUP), :]
                for kb in range(width // LANES)
            ],
            axis=1,
        )
        out = lax.dot_general(lhs, w1[...], nt, preferred_element_type=jnp.float32)
        foc[pl.ds(first, GROUP), :] = out.astype(jnp.bfloat16)
        for d in range(per1):
            dest = g * per1 + d

            @pl.when(dest != me)
            def _():
                copy1(0, dest, me).start()

    for h in range(1, halves):

        @pl.loop(0, groups1)
        def _(n):
            for d in range(per1):
                dest = order(n, own1, groups1) * per1 + d

                @pl.when(dest != me)
                def _():
                    copy1(h, dest, me).start()

    for h in range(halves):
        foc_in[h, me] = foc[pl.ds(pl.multiple_of(me * cols + h * hc, hc), hc), :]
    loads[2].wait()
    skew(staps_ref, padded, False, rows, band_s)

    groups2 = sources // GROUP
    per2 = GROUP // rows
    own2 = me // per2
    lane = lax.broadcasted_iota(jnp.int32, (hc, 2 * rows), 1)
    for h in range(halves):
        drain(foc_in.at[h, pl.ds(0, panels - 1)], recv1.at[h])
        for j in range(panels):
            x = foc_in[h, j]
            at = 2 * rows * j
            w2[0:hc, at : at + 2 * rows] = jnp.where(lane < rows, x, -x)
            w2[hc : 2 * hc, at : at + 2 * rows] = jnp.concatenate([x[:, rows:], x[:, :rows]], axis=1)

        @pl.loop(0, groups2)
        def _(n):
            g = order(n, own2, groups2)
            first = pl.multiple_of(g * GROUP, GROUP)
            lhs = jnp.concatenate(
                [
                    band_s[pl.ds(pl.multiple_of(sources - rows * (jb + 1) + first, rows), GROUP), :]
                    for jb in range(panels)
                ],
                axis=1,
            )
            out = lax.dot_general(lhs, w2[...], nt, preferred_element_type=jnp.float32)
            mul[h, pl.ds(first, GROUP), :] = out.astype(jnp.bfloat16)
            for d in range(per2):
                dest = g * per2 + d

                @pl.when(dest != me)
                def _():
                    copy2(h, dest, me).start()

        mul_in[h, me] = mul[h, pl.ds(pl.multiple_of(me * rows, rows), rows), :]

    def fold(v):
        return jnp.sum(v, axis=0, keepdims=True)

    near = LANES // cols
    chunks = side // near

    def gather(q, count, acc):
        if count:
            drain(mul_in.at[:, pl.ds(q * side, count)], recv2.at[q])

        def step(n, acc):
            cb = q * chunks + n
            blocks = [mul_in[h, cb * near + d] for d in range(near) for h in range(halves)]
            mre = jnp.concatenate([b[:, :hc] for b in blocks], axis=1)
            mim = jnp.concatenate([b[:, hc:] for b in blocks], axis=1)
            at = pl.ds(pl.multiple_of(cb * LANES, LANES), LANES)
            mult_ref[0, 0, :, at] = mre
            mult_ref[0, 1, :, at] = mim
            mre = mre.astype(jnp.float32)
            mim = mim.astype(jnp.float32)
            pre = rec_ref[0, 0, :, at]
            pim = rec_ref[0, 1, :, at]
            return (
                acc[0] + fold(mre * pre + mim * pim),
                acc[1] + fold(mre * pim - mim * pre),
                acc[2] + fold(mre * mre + mim * mim),
            )

        return lax.fori_loop(0, chunks, step, acc)

    zero = jnp.zeros((1, LANES), jnp.float32)
    sides = gather(plane, side - 1, (zero, zero, zero))

    def visit(n, acc):
        p = jnp.where(plane < planes // 2, plane, planes - 1 - plane)
        q = jnp.where(n < planes // 2 - 1, n + (n >= p), planes + planes // 2 - 2 - n)
        return gather(jnp.where(plane < planes // 2, q, planes - 1 - q), side, acc)

    num_re, num_im, energy = lax.fori_loop(0, planes - 1, visit, sides)
    part = jnp.concatenate([num_re, num_im, energy, jnp.zeros((5, LANES), jnp.float32)], axis=0)
    sums[...] = part
    sums_in[me] = part

    @pl.loop(1, panels)
    def _(o):
        copy3(peer(o), me).start()

    drain(foc.at[pl.ds(0, width - cols), :], send1)
    drain(mul.at[:, pl.ds(0, sources - rows), :], send2)
    drain(sums_in.at[pl.ds(0, panels - 1)], recv3)
    drain(sums_in.at[pl.ds(0, panels - 1)], send3)

    total = jnp.sum(jnp.sum(sums_in[...], axis=0), axis=1, keepdims=True)
    fit = total[0:2, :] / (total[2:3, :] + 1e-06)
    fit_ref[...] = jnp.broadcast_to(
        jnp.concatenate([fit, jnp.zeros((6, 1), jnp.float32)], axis=0), (8, LANES)
    )


def subtract_kernel(rec_ref, mult_ref, fit_ref, prim_hbm, mult_hbm, prim, sem):
    mult_out = pltpu.make_async_copy(mult_ref, mult_hbm, sem.at[0])
    mult_out.start()
    fit_re = fit_ref[0:1, 0:1]
    fit_im = fit_ref[1:2, 0:1]
    rows = rec_ref.shape[2]
    strip = rows // STRIPS
    outs = []
    for i in range(STRIPS):
        at = slice(i * strip, (i + 1) * strip)
        mre = mult_ref[0, 0, at, :].astype(jnp.float32)
        mim = mult_ref[0, 1, at, :].astype(jnp.float32)
        prim[0, 0, at, :] = rec_ref[0, 0, at, :] - (fit_re * mre - fit_im * mim)
        prim[0, 1, at, :] = rec_ref[0, 1, at, :] - (fit_re * mim + fit_im * mre)
        out = pltpu.make_async_copy(prim.at[:, :, at, :], prim_hbm.at[:, :, at, :], sem.at[i + 1])
        out.start()
        outs.append(out)
    for out in outs:
        out.wait()
    mult_out.wait()


def per_device(recorded, receiver_kernel, source_kernel):
    rows, width = recorded.shape[2], recorded.shape[3]
    panels = lax.axis_size("panel")
    sources = rows * panels
    cols = width // panels
    bf16 = jnp.bfloat16
    vmem = pl.BlockSpec(memory_space=pltpu.VMEM)
    hc = min(cols, LANES // 2)
    halves = cols // hc
    planes = PLANES if panels % PLANES == 0 else 1
    sem = pltpu.SemaphoreType.DMA
    hbm = pl.BlockSpec(memory_space=pltpu.HBM)
    rec, mult, fit = pl.pallas_call(
        functools.partial(exchange_kernel, panels),
        out_shape=(
            jax.ShapeDtypeStruct(recorded.shape, jnp.float32),
            jax.ShapeDtypeStruct(recorded.shape, bf16),
            jax.ShapeDtypeStruct((8, LANES), jnp.float32),
        ),
        in_specs=[hbm] * 3,
        out_specs=(vmem, vmem, vmem),
        scratch_shapes=[
            pltpu.VMEM(receiver_kernel.shape, bf16),
            pltpu.VMEM(source_kernel.shape, bf16),
            sem((3,)),
            pltpu.VMEM((2, 2 * width), jnp.float32),
            pltpu.VMEM((2 * width, 2 * LANES), bf16),
            pltpu.VMEM((2 * sources, 2 * rows), bf16),
            pltpu.VMEM((2 * rows, 2 * width), bf16),
            pltpu.VMEM((2 * hc, 2 * sources), bf16),
            pltpu.VMEM((width, 2 * rows), bf16),
            pltpu.VMEM((halves, panels, hc, 2 * rows), bf16),
            pltpu.VMEM((halves, sources, 2 * hc), bf16),
            pltpu.VMEM((halves, panels, rows, 2 * hc), bf16),
            pltpu.VMEM((8, LANES), jnp.float32),
            pltpu.VMEM((panels, 8, LANES), jnp.float32),
            sem,
            sem((halves,)),
            sem,
            sem((planes,)),
            sem,
            sem,
        ],
        compiler_params=pltpu.CompilerParams(collective_id=0, has_side_effects=True, vmem_limit_bytes=50 * 2**20),
        name="exchange",
    )(
        *(pltpu.with_memory_space_constraint(x, pltpu.HBM) for x in (recorded, receiver_kernel, source_kernel))
    )
    return pl.pallas_call(
        subtract_kernel,
        out_shape=(
            jax.ShapeDtypeStruct(recorded.shape, jnp.float32),
            jax.ShapeDtypeStruct(recorded.shape, bf16),
        ),
        in_specs=[vmem] * 3,
        out_specs=(hbm, hbm),
        scratch_shapes=[pltpu.VMEM(recorded.shape, jnp.float32), pltpu.SemaphoreType.DMA((STRIPS + 1,))],
        compiler_params=pltpu.CompilerParams(vmem_limit_bytes=12 * 2**20),
        name="subtract",
    )(rec, mult, fit)


def solution(mesh):
    placed = (P("freq", None, "panel", None), P("freq", None, None), P("freq", None, None))
    return jax.shard_map(
        per_device,
        mesh=mesh,
        in_specs=placed,
        out_specs=(P("freq", None, "panel", None), P("freq", None, "panel", None)),
        check_vma=False,
    )
```

```python
import functools

import jax
import jax.numpy as jnp
from jax import lax
from jax.experimental import pallas as pl
from jax.experimental.pallas import tpu as pltpu
from jax.sharding import PartitionSpec as P

MESH = pl.DeviceIdType.MESH
LANES = 128
GROUP = 256
STRIP = 16
STRIPS = 4
PLANES = 4


def spread(taps_ref, padded, comp, flipped):
    length = padded.shape[1]
    rows = [padded[comp : comp + 1, at : at + LANES] for at in range(0, length, LANES)]
    if not flipped:
        return jnp.broadcast_to(jnp.concatenate(rows, axis=1), (STRIP, length))
    i = lax.broadcasted_iota(jnp.int32, (LANES, LANES), 0)
    j = lax.broadcasted_iota(jnp.int32, (LANES, LANES), 1)
    swap = jnp.where(i + j == LANES - 1, 1.0, 0.0).astype(jnp.bfloat16)
    tall = jnp.concatenate([jnp.broadcast_to(r, (STRIP, LANES)) for r in rows[::-1]], axis=0)
    tall = jnp.dot(tall.astype(jnp.bfloat16), swap, preferred_element_type=jnp.float32)
    return jnp.concatenate([tall[at : at + STRIP] for at in range(0, tall.shape[0], STRIP)], axis=1)


def skew(taps_ref, padded, flipped, block, band_ref):
    length = padded.shape[1]
    padded[...] = jnp.zeros_like(padded)
    padded[:, 0 : length - 1] = taps_ref[0].astype(jnp.float32)
    row = lax.broadcasted_iota(jnp.int32, (STRIP, length), 0)
    for comp in range(2):
        x = spread(taps_ref, padded, comp, flipped)
        step = 1
        while step < STRIP:
            x = jnp.where((row & step) != 0, pltpu.roll(x, step, 1), x)
            step *= 2
        lane0 = comp * block
        for s in range(0, LANES, STRIP):
            shift = (s - (LANES - block) + (0 if flipped else 1)) % length
            y = (pltpu.roll(x, shift, 1) if shift else x).astype(jnp.bfloat16)
            for m in range(length // LANES):
                at = length - LANES * (m + 1)
                band_ref[m * LANES + s : m * LANES + s + STRIP, lane0 : lane0 + block] = y[:, at : at + block]


def exchange_kernel(
    panels,
    rec_hbm,
    rtaps_hbm,
    staps_hbm,
    rec_ref,
    mult_ref,
    fit_ref,
    rtaps_ref,
    staps_ref,
    load_sem,
    padded,
    band_r,
    band_s,
    w1,
    w2,
    foc,
    foc_in,
    mul,
    mul_in,
    sums,
    sums_in,
    send1,
    recv1,
    send2,
    recv2,
    send3,
    recv3,
    relay,
):
    me = lax.axis_index("panel")
    rows, width = rec_ref.shape[2], rec_ref.shape[3]
    sources = rows * panels
    cols = width // panels
    halves, hc = foc_in.shape[0], foc_in.shape[2]
    nt = (((1,), (1,)), ((), ()))
    planes = recv2.shape[0]
    side = panels // planes
    plane = me // side

    def order(n, own, groups, rev=0):
        half = groups // 2
        far = lax.rem(own // half + 1 + n // half, 2)
        at = lax.rem(n, half)
        at = jnp.where(far == 1 - rev, half - 1 - at, at)
        return far * half + at + jnp.where(lax.rem(at, 2) == 0, 1, -1) * lax.rem(own, 2)

    def peer(o):
        return lax.rem(me + o, panels)

    loads = [
        pltpu.make_async_copy(src, dst, load_sem.at[i])
        for i, (src, dst) in enumerate(
            ((rtaps_hbm, rtaps_ref), (rec_hbm, rec_ref), (staps_hbm, staps_ref))
        )
    ]
    for load in loads:
        load.start()

    barrier = pltpu.get_barrier_semaphore()

    @pl.loop(0, panels)
    def _(o):
        gap = jnp.abs(o // side - plane)

        @pl.when(jnp.logical_and(gap <= 1, o != me))
        def _():
            pl.semaphore_signal(barrier, inc=1, device_id={"panel": o}, device_id_type=MESH)

    above = (plane > 0).astype(jnp.int32)
    below = (plane < planes - 1).astype(jnp.int32)

    outer = jnp.logical_or(plane == 0, plane == planes - 1)
    inner = jnp.logical_not(outer)
    outward = jnp.where(plane * 2 < planes, -side, side)
    inward = -outward

    def tell(slot, step):
        pl.semaphore_signal(relay.at[slot], inc=1, device_id={"panel": me + step}, device_id_type=MESH)

    loads[0].wait()
    skew(rtaps_ref, padded, True, LANES, band_r)
    loads[1].wait()
    for kb in range(width // LANES):
        re = rec_ref[0, 0, :, kb * LANES : (kb + 1) * LANES].astype(jnp.bfloat16)
        im = rec_ref[0, 1, :, kb * LANES : (kb + 1) * LANES].astype(jnp.bfloat16)
        at = 2 * kb * LANES
        w1[0:rows, at : at + LANES] = re
        w1[0:rows, at + LANES : at + 2 * LANES] = -im
        w1[rows : 2 * rows, at : at + LANES] = im
        w1[rows : 2 * rows, at + LANES : at + 2 * LANES] = re

    pl.semaphore_wait(barrier, side * (1 + above + below) - 1)
    if planes > 1:

        @pl.when(inner)
        def _():
            tell(0, inward)
            tell(1, outward)

    def copy1(h, dest, src):
        return pltpu.make_async_remote_copy(
            src_ref=foc.at[pl.ds(pl.multiple_of(dest * cols + h * hc, hc), hc), :],
            dst_ref=foc_in.at[h, src],
            send_sem=send1,
            recv_sem=recv1.at[h],
            device_id={"panel": dest},
            device_id_type=MESH,
        )

    def copy2(h, dest, src):
        return pltpu.make_async_remote_copy(
            src_ref=mul.at[h, pl.ds(pl.multiple_of(dest * rows, rows), rows), :],
            dst_ref=mul_in.at[h, src],
            send_sem=send2,
            recv_sem=recv2.at[src // side],
            device_id={"panel": dest},
            device_id_type=MESH,
        )

    def drain(ref, sem):
        pltpu.make_async_copy(ref, ref, sem).wait()

    def copy3(dest, src):
        return pltpu.make_async_remote_copy(
            src_ref=sums,
            dst_ref=sums_in.at[src],
            send_sem=send3,
            recv_sem=recv3,
            device_id={"panel": dest},
            device_id_type=MESH,
        )

    groups1 = width // GROUP
    per1 = GROUP // cols
    own1 = me // per1

    @pl.loop(0, groups1)
    def _(n):
        g = order(n, own1, groups1, 1)
        if planes > 1:

            @pl.when(jnp.logical_and(inner, n == groups1 // planes))
            def _():
                pl.semaphore_wait(relay.at[0], 1)
                tell(2, outward)

        first = pl.multiple_of(g * GROUP, GROUP)
        lhs = jnp.concatenate(
            [
                band_r[pl.ds(pl.multiple_of(width - LANES * (kb + 1) + first, LANES), GROUP), :]
                for kb in range(width // LANES)
            ],
            axis=1,
        )
        out = lax.dot_general(lhs, w1[...], nt, preferred_element_type=jnp.float32)
        foc[pl.ds(first, GROUP), :] = out.astype(jnp.bfloat16)
        if planes > 1:

            @pl.when(jnp.logical_and(outer, n == 0))
            def _():
                pl.semaphore_wait(relay.at[1], 1)

            @pl.when(jnp.logical_and(outer, n == groups1 // planes))
            def _():
                pl.semaphore_wait(relay.at[2], 1)

        for d in range(per1):
            dest = g * per1 + d

            @pl.when(dest != me)
            def _():
                copy1(0, dest, me).start()

    for h in range(1, halves):

        @pl.loop(0, groups1)
        def _(n):
            for d in range(per1):
                dest = order(n, own1, groups1, 1) * per1 + d

                @pl.when(dest != me)
                def _():
                    copy1(h, dest, me).start()

    for h in range(halves):
        foc_in[h, me] = foc[pl.ds(pl.multiple_of(me * cols + h * hc, hc), hc), :]
    loads[2].wait()
    skew(staps_ref, padded, False, rows, band_s)

    groups2 = sources // GROUP
    per2 = GROUP // rows
    own2 = me // per2
    lane = lax.broadcasted_iota(jnp.int32, (hc, 2 * rows), 1)
    for h in range(halves):
        drain(foc_in.at[h, pl.ds(0, panels - 1)], recv1.at[h])
        for j in range(panels):
            x = foc_in[h, j]
            at = 2 * rows * j
            w2[0:hc, at : at + 2 * rows] = jnp.where(lane < rows, x, -x)
            w2[hc : 2 * hc, at : at + 2 * rows] = jnp.concatenate([x[:, rows:], x[:, :rows]], axis=1)

        @pl.loop(0, groups2)
        def _(n):
            g = order(n, own2, groups2)
            first = pl.multiple_of(g * GROUP, GROUP)
            lhs = jnp.concatenate(
                [
                    band_s[pl.ds(pl.multiple_of(sources - rows * (jb + 1) + first, rows), GROUP), :]
                    for jb in range(panels)
                ],
                axis=1,
            )
            out = lax.dot_general(lhs, w2[...], nt, preferred_element_type=jnp.float32)
            mul[h, pl.ds(first, GROUP), :] = out.astype(jnp.bfloat16)
            for d in range(per2):
                dest = g * per2 + d

                @pl.when(dest != me)
                def _():
                    copy2(h, dest, me).start()

        mul_in[h, me] = mul[h, pl.ds(pl.multiple_of(me * rows, rows), rows), :]

    def fold(v):
        return jnp.sum(v, axis=0, keepdims=True)

    near = LANES // cols
    chunks = side // near

    def gather(q, count, acc):
        if count:
            drain(mul_in.at[:, pl.ds(q * side, count)], recv2.at[q])

        def step(n, acc):
            cb = q * chunks + n
            blocks = [mul_in[h, cb * near + d] for d in range(near) for h in range(halves)]
            mre = jnp.concatenate([b[:, :hc] for b in blocks], axis=1)
            mim = jnp.concatenate([b[:, hc:] for b in blocks], axis=1)
            at = pl.ds(pl.multiple_of(cb * LANES, LANES), LANES)
            mult_ref[0, 0, :, at] = mre
            mult_ref[0, 1, :, at] = mim
            mre = mre.astype(jnp.float32)
            mim = mim.astype(jnp.float32)
            pre = rec_ref[0, 0, :, at]
            pim = rec_ref[0, 1, :, at]
            return (
                acc[0] + fold(mre * pre + mim * pim),
                acc[1] + fold(mre * pim - mim * pre),
                acc[2] + fold(mre * mre + mim * mim),
            )

        return lax.fori_loop(0, chunks, step, acc)

    zero = jnp.zeros((1, LANES), jnp.float32)
    sides = gather(plane, side - 1, (zero, zero, zero))

    def visit(n, acc):
        p = jnp.where(plane < planes // 2, plane, planes - 1 - plane)
        q = jnp.where(n < planes // 2 - 1, n + (n >= p), planes + planes // 2 - 2 - n)
        return gather(jnp.where(plane < planes // 2, q, planes - 1 - q), side, acc)

    num_re, num_im, energy = lax.fori_loop(0, planes - 1, visit, sides)
    part = jnp.concatenate([num_re, num_im, energy, jnp.zeros((5, LANES), jnp.float32)], axis=0)
    sums[...] = part
    sums_in[me] = part

    @pl.loop(1, panels)
    def _(o):
        copy3(peer(o), me).start()

    drain(foc.at[pl.ds(0, width - cols), :], send1)
    drain(mul.at[:, pl.ds(0, sources - rows), :], send2)
    drain(sums_in.at[pl.ds(0, panels - 1)], recv3)
    drain(sums_in.at[pl.ds(0, panels - 1)], send3)

    total = jnp.sum(jnp.sum(sums_in[...], axis=0), axis=1, keepdims=True)
    fit = total[0:2, :] / (total[2:3, :] + 1e-06)
    fit_ref[...] = jnp.broadcast_to(
        jnp.concatenate([fit, jnp.zeros((6, 1), jnp.float32)], axis=0), (8, LANES)
    )


def subtract_kernel(rec_ref, mult_ref, fit_ref, prim_hbm, mult_hbm, prim, sem):
    mult_out = pltpu.make_async_copy(mult_ref, mult_hbm, sem.at[0])
    mult_out.start()
    fit_re = fit_ref[0:1, 0:1]
    fit_im = fit_ref[1:2, 0:1]
    rows = rec_ref.shape[2]
    strip = rows // STRIPS
    outs = []
    for i in range(STRIPS):
        at = slice(i * strip, (i + 1) * strip)
        mre = mult_ref[0, 0, at, :].astype(jnp.float32)
        mim = mult_ref[0, 1, at, :].astype(jnp.float32)
        prim[0, 0, at, :] = rec_ref[0, 0, at, :] - (fit_re * mre - fit_im * mim)
        prim[0, 1, at, :] = rec_ref[0, 1, at, :] - (fit_re * mim + fit_im * mre)
        out = pltpu.make_async_copy(prim.at[:, :, at, :], prim_hbm.at[:, :, at, :], sem.at[i + 1])
        out.start()
        outs.append(out)
    for out in outs:
        out.wait()
    mult_out.wait()


def per_device(recorded, receiver_kernel, source_kernel):
    rows, width = recorded.shape[2], recorded.shape[3]
    panels = lax.axis_size("panel")
    sources = rows * panels
    cols = width // panels
    bf16 = jnp.bfloat16
    vmem = pl.BlockSpec(memory_space=pltpu.VMEM)
    hc = min(cols, LANES // 2)
    halves = cols // hc
    planes = PLANES if panels % PLANES == 0 else 1
    sem = pltpu.SemaphoreType.DMA
    hbm = pl.BlockSpec(memory_space=pltpu.HBM)
    rec, mult, fit = pl.pallas_call(
        functools.partial(exchange_kernel, panels),
        out_shape=(
            jax.ShapeDtypeStruct(recorded.shape, jnp.float32),
            jax.ShapeDtypeStruct(recorded.shape, bf16),
            jax.ShapeDtypeStruct((8, LANES), jnp.float32),
        ),
        in_specs=[hbm] * 3,
        out_specs=(vmem, vmem, vmem),
        scratch_shapes=[
            pltpu.VMEM(receiver_kernel.shape, bf16),
            pltpu.VMEM(source_kernel.shape, bf16),
            sem((3,)),
            pltpu.VMEM((2, 2 * width), jnp.float32),
            pltpu.VMEM((2 * width, 2 * LANES), bf16),
            pltpu.VMEM((2 * sources, 2 * rows), bf16),
            pltpu.VMEM((2 * rows, 2 * width), bf16),
            pltpu.VMEM((2 * hc, 2 * sources), bf16),
            pltpu.VMEM((width, 2 * rows), bf16),
            pltpu.VMEM((halves, panels, hc, 2 * rows), bf16),
            pltpu.VMEM((halves, sources, 2 * hc), bf16),
            pltpu.VMEM((halves, panels, rows, 2 * hc), bf16),
            pltpu.VMEM((8, LANES), jnp.float32),
            pltpu.VMEM((panels, 8, LANES), jnp.float32),
            sem,
            sem((halves,)),
            sem,
            sem((planes,)),
            sem,
            sem,
            pltpu.SemaphoreType.REGULAR((3,)),
        ],
        compiler_params=pltpu.CompilerParams(collective_id=0, has_side_effects=True, vmem_limit_bytes=50 * 2**20),
        name="exchange",
    )(
        *(pltpu.with_memory_space_constraint(x, pltpu.HBM) for x in (recorded, receiver_kernel, source_kernel))
    )
    return pl.pallas_call(
        subtract_kernel,
        out_shape=(
            jax.ShapeDtypeStruct(recorded.shape, jnp.float32),
            jax.ShapeDtypeStruct(recorded.shape, bf16),
        ),
        in_specs=[vmem] * 3,
        out_specs=(hbm, hbm),
        scratch_shapes=[pltpu.VMEM(recorded.shape, jnp.float32), pltpu.SemaphoreType.DMA((STRIPS + 1,))],
        compiler_params=pltpu.CompilerParams(vmem_limit_bytes=12 * 2**20),
        name="subtract",
    )(rec, mult, fit)


def solution(mesh):
    placed = (P("freq", None, "panel", None), P("freq", None, None), P("freq", None, None))
    return jax.shard_map(
        per_device,
        mesh=mesh,
        in_specs=placed,
        out_specs=(P("freq", None, "panel", None), P("freq", None, "panel", None)),
        check_vma=False,
    )
```

```python
import functools

import jax
import jax.numpy as jnp
from jax import lax
from jax.experimental import pallas as pl
from jax.experimental.pallas import tpu as pltpu
from jax.sharding import PartitionSpec as P

MESH = pl.DeviceIdType.MESH
LANES = 128
GROUP = 256
STRIP = 16
STRIPS = 4
PLANES = 4
INNER1 = True
CROSS1 = 1
INNER2 = False
CROSS2 = 1


def spread(taps_ref, padded, comp, flipped):
    length = padded.shape[1]
    rows = [padded[comp : comp + 1, at : at + LANES] for at in range(0, length, LANES)]
    if not flipped:
        return jnp.broadcast_to(jnp.concatenate(rows, axis=1), (STRIP, length))
    i = lax.broadcasted_iota(jnp.int32, (LANES, LANES), 0)
    j = lax.broadcasted_iota(jnp.int32, (LANES, LANES), 1)
    swap = jnp.where(i + j == LANES - 1, 1.0, 0.0).astype(jnp.bfloat16)
    tall = jnp.concatenate([jnp.broadcast_to(r, (STRIP, LANES)) for r in rows[::-1]], axis=0)
    tall = jnp.dot(tall.astype(jnp.bfloat16), swap, preferred_element_type=jnp.float32)
    return jnp.concatenate([tall[at : at + STRIP] for at in range(0, tall.shape[0], STRIP)], axis=1)


def skew(taps_ref, padded, flipped, block, band_ref):
    length = padded.shape[1]
    padded[...] = jnp.zeros_like(padded)
    padded[:, 0 : length - 1] = taps_ref[0].astype(jnp.float32)
    row = lax.broadcasted_iota(jnp.int32, (STRIP, length), 0)
    for comp in range(2):
        x = spread(taps_ref, padded, comp, flipped)
        x = pltpu.roll(x, 0, 1, stride=1, stride_axis=0)
        lane0 = comp * block
        xb = x.astype(jnp.bfloat16)
        for s in range(0, LANES, STRIP):
            shift = (s - (LANES - block) + (0 if flipped else 1)) % length
            y = jnp.concatenate([xb[:, length - shift :], xb[:, : length - shift]], axis=1) if shift else xb
            for m in range(length // LANES):
                at = length - LANES * (m + 1)
                band_ref[m * LANES + s : m * LANES + s + STRIP, lane0 : lane0 + block] = y[:, at : at + block]


def exchange_kernel(
    panels,
    planes,
    rec_hbm,
    rtaps_hbm,
    staps_hbm,
    rec_ref,
    mult_ref,
    fit_ref,
    rtaps_ref,
    staps_ref,
    load_sem,
    padded,
    band_r,
    band_s,
    w1,
    w2,
    foc,
    foc_in,
    mul,
    mul_in,
    sums,
    sums_in,
    send1,
    recv1,
    send2,
    recv2,
    send3,
    recv3,
    relay,
):
    me = lax.axis_index("panel")
    rows, width = rec_ref.shape[2], rec_ref.shape[3]
    sources = rows * panels
    cols = width // panels
    halves, hc = foc_in.shape[0], foc_in.shape[2]
    nt = (((1,), (1,)), ((), ()))
    side = panels // planes
    plane = me // side

    def order(n, own, groups, inner_first, cross):
        wide = groups // planes
        high = own // wide >= planes // 2
        m = n // wide
        if inner_first:
            q = jnp.where(m < planes // 2, planes // 2 + m, planes - 1 - m)
        else:
            q = jnp.where(m < planes // 2, planes - 1 - m, m - planes // 2)
        q = jnp.where(high, planes - 1 - q, q)
        return q * wide + lax.rem(lax.rem(own, wide) + cross + n, wide)

    def peer(o):
        return lax.rem(me + o, panels)

    loads = [
        pltpu.make_async_copy(src, dst, load_sem.at[i])
        for i, (src, dst) in enumerate(
            ((rtaps_hbm, rtaps_ref), (rec_hbm, rec_ref), (staps_hbm, staps_ref))
        )
    ]
    for load in loads[:2]:
        load.start()

    barrier = pltpu.get_barrier_semaphore()

    @pl.loop(jnp.maximum(plane - 1, 0) * side, jnp.minimum(plane + 2, planes) * side)
    def _(o):
        @pl.when(o != me)
        def _():
            pl.semaphore_signal(barrier, inc=1, device_id={"panel": o}, device_id_type=MESH)

    above = (plane > 0).astype(jnp.int32)
    below = (plane < planes - 1).astype(jnp.int32)

    outer = jnp.logical_or(plane == 0, plane == planes - 1)
    inner = jnp.logical_not(outer)
    outward = jnp.where(plane * 2 < planes, -side, side)
    inward = -outward

    def tell(slot, step):
        pl.semaphore_signal(relay.at[slot], inc=1, device_id={"panel": me + step}, device_id_type=MESH)

    loads[0].wait()
    skew(rtaps_ref, padded, True, LANES, band_r)
    loads[2].start()
    loads[1].wait()
    for comp in range(2):
        w1[comp * rows : (comp + 1) * rows, :] = rec_ref[0, comp].astype(jnp.bfloat16)

    pl.semaphore_wait(barrier, side * (1 + above + below) - 1)
    if planes > 1:

        @pl.when(inner)
        def _():
            tell(0, inward)
            tell(1, outward)

    def copy1(h, dest, src):
        return pltpu.make_async_remote_copy(
            src_ref=foc.at[pl.ds(pl.multiple_of(dest * cols + h * hc, hc), hc), :],
            dst_ref=foc_in.at[h, src],
            send_sem=send1,
            recv_sem=recv1.at[h],
            device_id={"panel": dest},
            device_id_type=MESH,
        )

    def copy2(h, dest, src):
        return pltpu.make_async_remote_copy(
            src_ref=mul.at[h, pl.ds(pl.multiple_of(dest * rows, rows), rows), :],
            dst_ref=mul_in.at[h, src],
            send_sem=send2,
            recv_sem=recv2.at[src // per2],
            device_id={"panel": dest},
            device_id_type=MESH,
        )

    def drain(ref, sem):
        pltpu.make_async_copy(ref, ref, sem).wait()

    def copy3(dest, src):
        return pltpu.make_async_remote_copy(
            src_ref=sums,
            dst_ref=sums_in.at[src],
            send_sem=send3,
            recv_sem=recv3,
            device_id={"panel": dest},
            device_id_type=MESH,
        )

    groups1 = width // GROUP
    per1 = GROUP // cols
    own1 = me // per1

    @pl.loop(0, groups1)
    def _(n):
        g = order(n, own1, groups1, INNER1, CROSS1)
        if planes > 1:

            @pl.when(jnp.logical_and(inner, n == groups1 // planes))
            def _():
                pl.semaphore_wait(relay.at[0], 1)
                tell(2, outward)

        first = pl.multiple_of(g * GROUP, GROUP)
        parts = []
        for comp in range(2):
            lhs = jnp.concatenate(
                [
                    band_r[
                        pl.ds(pl.multiple_of(width - LANES * (kb + 1) + first, LANES), GROUP),
                        comp * LANES : (comp + 1) * LANES,
                    ]
                    for kb in range(width // LANES)
                ],
                axis=1,
            )
            parts.append(lax.dot_general(lhs, w1[...], nt, preferred_element_type=jnp.float32))
        re, im = parts
        out = jnp.concatenate([re[:, :rows] - im[:, rows:], re[:, rows:] + im[:, :rows]], axis=1)
        foc[pl.ds(first, GROUP), :] = out.astype(jnp.bfloat16)
        if planes > 1:

            @pl.when(jnp.logical_and(outer, n == 0))
            def _():
                pl.semaphore_wait(relay.at[1], 1)

            @pl.when(jnp.logical_and(outer, n == groups1 // planes))
            def _():
                pl.semaphore_wait(relay.at[2], 1)

        for d in range(per1):
            dest = g * per1 + d

            @pl.when(dest != me)
            def _():
                copy1(0, dest, me).start()

    for h in range(1, halves):

        @pl.loop(0, groups1)
        def _(n):
            for d in range(per1):
                dest = order(n, own1, groups1, INNER1, CROSS1) * per1 + d

                @pl.when(dest != me)
                def _():
                    copy1(h, dest, me).start()

    for h in range(halves):
        foc_in[h, me] = foc[pl.ds(pl.multiple_of(me * cols + h * hc, hc), hc), :]
    loads[2].wait()
    skew(staps_ref, padded, False, rows, band_s)

    groups2 = sources // GROUP
    per2 = GROUP // rows
    own2 = me // per2
    lane = lax.broadcasted_iota(jnp.int32, (hc, 2 * rows), 1)
    for h in range(halves):
        drain(foc_in.at[h, pl.ds(0, panels - 1)], recv1.at[h])
        for j in range(panels):
            x = foc_in[h, j]
            at = 2 * rows * j
            w2[0:hc, at : at + 2 * rows] = jnp.where(lane < rows, x, -x)
            w2[hc : 2 * hc, at : at + 2 * rows] = jnp.concatenate([x[:, rows:], x[:, :rows]], axis=1)

        @pl.loop(0, groups2)
        def _(n):
            g = order(n, own2, groups2, INNER2, CROSS2)
            first = pl.multiple_of(g * GROUP, GROUP)
            lhs = jnp.concatenate(
                [
                    band_s[pl.ds(pl.multiple_of(sources - rows * (jb + 1) + first, rows), GROUP), :]
                    for jb in range(panels)
                ],
                axis=1,
            )
            out = lax.dot_general(lhs, w2[...], nt, preferred_element_type=jnp.float32)
            mul[h, pl.ds(first, GROUP), :] = out.astype(jnp.bfloat16)
            for d in range(per2):
                dest = g * per2 + d

                @pl.when(dest != me)
                def _():
                    copy2(h, dest, me).start()

        mul_in[h, me] = mul[h, pl.ds(pl.multiple_of(me * rows, rows), rows), :]

    def fold(v):
        return jnp.sum(v, axis=0, keepdims=True)

    near = LANES // cols
    chunks = per2 // near

    def gather(q, count, acc):
        if count:
            drain(mul_in.at[:, pl.ds(q * per2, count)], recv2.at[q])

        def step(n, acc):
            cb = q * chunks + n
            blocks = [mul_in[h, cb * near + d] for d in range(near) for h in range(halves)]
            mre = jnp.concatenate([b[:, :hc] for b in blocks], axis=1)
            mim = jnp.concatenate([b[:, hc:] for b in blocks], axis=1)
            at = pl.ds(pl.multiple_of(cb * LANES, LANES), LANES)
            mult_ref[0, 0, :, at] = mre
            mult_ref[0, 1, :, at] = mim
            mre = mre.astype(jnp.float32)
            mim = mim.astype(jnp.float32)
            pre = rec_ref[0, 0, :, at]
            pim = rec_ref[0, 1, :, at]
            return (
                acc[0] + fold(mre * pre + mim * pim),
                acc[1] + fold(mre * pim - mim * pre),
                acc[2] + fold(mre * mre + mim * mim),
            )

        return lax.fori_loop(0, chunks, step, acc)

    zero = jnp.zeros((1, LANES), jnp.float32)
    wide = groups2 // planes
    place = own2 - plane * wide

    def visit(n, acc):
        m = n // wide
        p = jnp.where(plane < planes // 2, plane, planes - 1 - plane)
        q = jnp.where(m == 0, p, jnp.where(m < planes // 2, m - (m <= p), planes + planes // 2 - 1 - m))
        q = jnp.where(plane < planes // 2, q, planes - 1 - q)
        at = lax.rem(n, wide)
        return gather(q * wide + jnp.where(m == 0, lax.rem(place + at, wide), lax.rem(place + 1 + at, wide)), per2, acc)

    num_re, num_im, energy = lax.fori_loop(1, groups2, visit, gather(own2, per2 - 1, (zero, zero, zero)))
    part = jnp.concatenate([num_re, num_im, energy, jnp.zeros((5, LANES), jnp.float32)], axis=0)
    sums[...] = part
    sums_in[me] = part

    @pl.loop(1, panels)
    def _(o):
        copy3(peer(o), me).start()

    drain(foc.at[pl.ds(0, width - cols), :], send1)
    drain(mul.at[:, pl.ds(0, sources - rows), :], send2)
    drain(sums_in.at[pl.ds(0, panels - 1)], recv3)
    drain(sums_in.at[pl.ds(0, panels - 1)], send3)

    total = jnp.sum(jnp.sum(sums_in[...], axis=0), axis=1, keepdims=True)
    fit = total[0:2, :] / (total[2:3, :] + 1e-06)
    fit_ref[...] = jnp.broadcast_to(
        jnp.concatenate([fit, jnp.zeros((6, 1), jnp.float32)], axis=0), (8, LANES)
    )


def subtract_kernel(rec_ref, mult_ref, fit_ref, prim_hbm, mult_hbm, prim, sem):
    mult_out = pltpu.make_async_copy(mult_ref, mult_hbm, sem.at[0])
    mult_out.start()
    fit_re = fit_ref[0:1, 0:1]
    fit_im = fit_ref[1:2, 0:1]
    rows = rec_ref.shape[2]
    strip = rows // STRIPS
    outs = []
    for i in range(STRIPS):
        at = slice(i * strip, (i + 1) * strip)
        mre = mult_ref[0, 0, at, :].astype(jnp.float32)
        mim = mult_ref[0, 1, at, :].astype(jnp.float32)
        prim[0, 0, at, :] = rec_ref[0, 0, at, :] - (fit_re * mre - fit_im * mim)
        prim[0, 1, at, :] = rec_ref[0, 1, at, :] - (fit_re * mim + fit_im * mre)
        out = pltpu.make_async_copy(prim.at[:, :, at, :], prim_hbm.at[:, :, at, :], sem.at[i + 1])
        out.start()
        outs.append(out)
    for out in outs:
        out.wait()
    mult_out.wait()


def per_device(recorded, receiver_kernel, source_kernel):
    rows, width = recorded.shape[2], recorded.shape[3]
    panels = lax.axis_size("panel")
    sources = rows * panels
    cols = width // panels
    bf16 = jnp.bfloat16
    vmem = pl.BlockSpec(memory_space=pltpu.VMEM)
    hc = min(cols, LANES // 2)
    halves = cols // hc
    planes = PLANES if (width // GROUP) % PLANES == 0 and (sources // GROUP) % PLANES == 0 else 1
    sem = pltpu.SemaphoreType.DMA
    hbm = pl.BlockSpec(memory_space=pltpu.HBM)
    rec, mult, fit = pl.pallas_call(
        functools.partial(exchange_kernel, panels, planes),
        out_shape=(
            jax.ShapeDtypeStruct(recorded.shape, jnp.float32),
            jax.ShapeDtypeStruct(recorded.shape, bf16),
            jax.ShapeDtypeStruct((8, LANES), jnp.float32),
        ),
        in_specs=[hbm] * 3,
        out_specs=(vmem, vmem, vmem),
        scratch_shapes=[
            pltpu.VMEM(receiver_kernel.shape, bf16),
            pltpu.VMEM(source_kernel.shape, bf16),
            sem((3,)),
            pltpu.VMEM((2, 2 * width), jnp.float32),
            pltpu.VMEM((2 * width, 2 * LANES), bf16),
            pltpu.VMEM((2 * sources, 2 * rows), bf16),
            pltpu.VMEM((2 * rows, width), bf16),
            pltpu.VMEM((2 * hc, 2 * sources), bf16),
            pltpu.VMEM((width, 2 * rows), bf16),
            pltpu.VMEM((halves, panels, hc, 2 * rows), bf16),
            pltpu.VMEM((halves, sources, 2 * hc), bf16),
            pltpu.VMEM((halves, panels, rows, 2 * hc), bf16),
            pltpu.VMEM((8, LANES), jnp.float32),
            pltpu.VMEM((panels, 8, LANES), jnp.float32),
            sem,
            sem((halves,)),
            sem,
            sem((sources // GROUP,)),
            sem,
            sem,
            pltpu.SemaphoreType.REGULAR((3,)),
        ],
        compiler_params=pltpu.CompilerParams(collective_id=0, has_side_effects=True, vmem_limit_bytes=50 * 2**20),
        name="exchange",
    )(
        *(pltpu.with_memory_space_constraint(x, pltpu.HBM) for x in (recorded, receiver_kernel, source_kernel))
    )
    return pl.pallas_call(
        subtract_kernel,
        out_shape=(
            jax.ShapeDtypeStruct(recorded.shape, jnp.float32),
            jax.ShapeDtypeStruct(recorded.shape, bf16),
        ),
        in_specs=[vmem] * 3,
        out_specs=(hbm, hbm),
        scratch_shapes=[pltpu.VMEM(recorded.shape, jnp.float32), pltpu.SemaphoreType.DMA((STRIPS + 1,))],
        compiler_params=pltpu.CompilerParams(vmem_limit_bytes=12 * 2**20),
        name="subtract",
    )(rec, mult, fit)


def solution(mesh):
    placed = (P("freq", None, "panel", None), P("freq", None, None), P("freq", None, None))
    return jax.shard_map(
        per_device,
        mesh=mesh,
        in_specs=placed,
        out_specs=(P("freq", None, "panel", None), P("freq", None, "panel", None)),
        check_vma=False,
    )
```

```python
import functools

import jax
import jax.numpy as jnp
from jax import lax
from jax.experimental import pallas as pl
from jax.experimental.pallas import tpu as pltpu
from jax.sharding import PartitionSpec as P

MESH = pl.DeviceIdType.MESH
LANES = 128
GROUP = 256
STRIP = 16
SUBLANES = 8
STRIPS = 4
PLANES = 4
INNER1 = True
CROSS1 = 0
INNER2 = False
CROSS2 = 1


def spread(taps_ref, padded, comp, flipped):
    length = padded.shape[1]
    rows = [padded[comp : comp + 1, at : at + LANES] for at in range(0, length, LANES)]
    if not flipped:
        return jnp.broadcast_to(jnp.concatenate(rows, axis=1), (STRIP, length))
    i = lax.broadcasted_iota(jnp.int32, (LANES, LANES), 0)
    j = lax.broadcasted_iota(jnp.int32, (LANES, LANES), 1)
    swap = jnp.where(i + j == LANES - 1, 1.0, 0.0).astype(jnp.bfloat16)
    tall = jnp.concatenate([jnp.broadcast_to(r, (SUBLANES, LANES)) for r in rows[::-1]], axis=0)
    tall = jnp.dot(tall.astype(jnp.bfloat16), swap, preferred_element_type=jnp.float32)
    x = jnp.concatenate([tall[at : at + SUBLANES] for at in range(0, tall.shape[0], SUBLANES)], axis=1)
    return jnp.concatenate([x] * (STRIP // SUBLANES), axis=0)


def skew(taps_ref, padded, flipped, block, band_ref):
    length = padded.shape[1]
    padded[...] = jnp.zeros_like(padded)
    padded[:, 0 : length - 1] = taps_ref[0].astype(jnp.float32)
    row = lax.broadcasted_iota(jnp.int32, (STRIP, length), 0)
    for comp in range(2):
        x = spread(taps_ref, padded, comp, flipped)
        x = pltpu.roll(x, 0, 1, stride=1, stride_axis=0)
        lane0 = comp * block
        xb = x.astype(jnp.bfloat16)
        for s in range(0, LANES, STRIP):
            shift = (s - (LANES - block) + (0 if flipped else 1)) % length
            y = jnp.concatenate([xb[:, length - shift :], xb[:, : length - shift]], axis=1) if shift else xb
            for m in range(length // LANES):
                at = length - LANES * (m + 1)
                band_ref[m * LANES + s : m * LANES + s + STRIP, lane0 : lane0 + block] = y[:, at : at + block]


def exchange_kernel(
    panels,
    planes,
    rec_hbm,
    rtaps_hbm,
    staps_hbm,
    rec_ref,
    mult_ref,
    fit_ref,
    rtaps_ref,
    staps_ref,
    load_sem,
    padded,
    band_r,
    band_s,
    w1,
    w2,
    foc,
    foc_in,
    mul,
    mul_in,
    sums,
    sums_in,
    send1,
    recv1,
    send2,
    recv2,
    send3,
    recv3,
    relay,
):
    me = lax.axis_index("panel")
    rows, width = rec_ref.shape[2], rec_ref.shape[3]
    sources = rows * panels
    cols = width // panels
    halves, hc = foc_in.shape[0], foc_in.shape[2]
    nt = (((1,), (1,)), ((), ()))
    side = panels // planes
    plane = me // side

    def order(n, own, groups, inner_first, cross):
        wide = groups // planes
        high = own // wide >= planes // 2
        m = n // wide
        if inner_first:
            q = jnp.where(m < planes // 2, planes // 2 + m, planes - 1 - m)
        else:
            q = jnp.where(m < planes // 2, planes - 1 - m, m - planes // 2)
        q = jnp.where(high, planes - 1 - q, q)
        return q * wide + lax.rem(lax.rem(own, wide) + cross + n, wide)

    def peer(o):
        return lax.rem(me + o, panels)

    loads = [
        pltpu.make_async_copy(src, dst, load_sem.at[i])
        for i, (src, dst) in enumerate(
            ((rtaps_hbm, rtaps_ref), (rec_hbm, rec_ref), (staps_hbm, staps_ref))
        )
    ]
    for load in loads[:2]:
        load.start()

    barrier = pltpu.get_barrier_semaphore()

    above = (plane > 0).astype(jnp.int32)
    below = (plane < planes - 1).astype(jnp.int32)
    groups1 = width // GROUP
    per1 = GROUP // cols
    own1 = me // per1
    wide1 = groups1 // planes

    def greet(o):
        pl.semaphore_signal(barrier, inc=1, device_id={"panel": o}, device_id_type=MESH)

    for d in range(per1):

        @pl.when(plane > 0)
        def _():
            greet(own1 * per1 - side + d)

        @pl.when(plane < planes - 1)
        def _():
            greet(own1 * per1 + side + d)

    @pl.loop(1, side)
    def _(o):
        greet(plane * side + lax.rem(me - plane * side + o, side))


    outer = jnp.logical_or(plane == 0, plane == planes - 1)
    inner = jnp.logical_not(outer)
    outward = jnp.where(plane * 2 < planes, -side, side)
    inward = -outward

    def tell(slot, step):
        pl.semaphore_signal(relay.at[slot], inc=1, device_id={"panel": me + step}, device_id_type=MESH)

    loads[0].wait()
    skew(rtaps_ref, padded, True, LANES, band_r)
    loads[2].start()
    loads[1].wait()
    for comp in range(2):
        w1[comp * rows : (comp + 1) * rows, :] = rec_ref[0, comp].astype(jnp.bfloat16)

    pl.semaphore_wait(barrier, side - 1 + per1 * (above + below))
    for k in range(1, wide1):
        dest = plane * side + lax.rem(me - plane * side + k * per1, side)
        pl.semaphore_signal(relay.at[3], inc=1, device_id={"panel": dest}, device_id_type=MESH)

    def copy1(h, dest, src):
        return pltpu.make_async_remote_copy(
            src_ref=foc.at[pl.ds(pl.multiple_of(dest * cols + h * hc, hc), hc), :],
            dst_ref=foc_in.at[h, src],
            send_sem=send1,
            recv_sem=recv1.at[h],
            device_id={"panel": dest},
            device_id_type=MESH,
        )

    def copy2(h, dest, src):
        return pltpu.make_async_remote_copy(
            src_ref=mul.at[h, pl.ds(pl.multiple_of(dest * rows, rows), rows), :],
            dst_ref=mul_in.at[h, src],
            send_sem=send2,
            recv_sem=recv2.at[src // per2],
            device_id={"panel": dest},
            device_id_type=MESH,
        )

    def drain(ref, sem):
        pltpu.make_async_copy(ref, ref, sem).wait()

    def copy3(dest, src):
        return pltpu.make_async_remote_copy(
            src_ref=sums,
            dst_ref=sums_in.at[src],
            send_sem=send3,
            recv_sem=recv3,
            device_id={"panel": dest},
            device_id_type=MESH,
        )

    @pl.loop(0, groups1)
    def _(n):
        g = order(n, own1, groups1, INNER1, CROSS1)
        if planes > 1:

            @pl.when(jnp.logical_and(inner, n == groups1 // planes))
            def _():
                pl.semaphore_wait(relay.at[0], 1)
                tell(2, outward)

        first = pl.multiple_of(g * GROUP, GROUP)
        parts = []
        for comp in range(2):
            lhs = jnp.concatenate(
                [
                    band_r[
                        pl.ds(pl.multiple_of(width - LANES * (kb + 1) + first, LANES), GROUP),
                        comp * LANES : (comp + 1) * LANES,
                    ]
                    for kb in range(width // LANES)
                ],
                axis=1,
            )
            parts.append(lax.dot_general(lhs, w1[...], nt, preferred_element_type=jnp.float32))
        re, im = parts
        out = jnp.concatenate([re[:, :rows] - im[:, rows:], re[:, rows:] + im[:, :rows]], axis=1)
        foc[pl.ds(first, GROUP), :] = out.astype(jnp.bfloat16)
        if planes > 1:

            @pl.when(jnp.logical_and(outer, n == 0))
            def _():
                pl.semaphore_wait(relay.at[1], 1)

            @pl.when(jnp.logical_and(outer, n == groups1 // planes))
            def _():
                pl.semaphore_wait(relay.at[2], 1)

        for d in range(per1):
            dest = g * per1 + d

            @pl.when(dest != me)
            def _():
                copy1(0, dest, me).start()

        @pl.when(n == 0)
        def _():
            if wide1 > 1:
                pl.semaphore_wait(relay.at[3], wide1 - 1)
            if planes > 1:

                @pl.when(inner)
                def _():
                    tell(0, inward)
                    tell(1, outward)

    for h in range(1, halves):

        @pl.loop(0, groups1)
        def _(n):
            for d in range(per1):
                dest = order(n, own1, groups1, INNER1, CROSS1) * per1 + d

                @pl.when(dest != me)
                def _():
                    copy1(h, dest, me).start()

    for h in range(halves):
        foc_in[h, me] = foc[pl.ds(pl.multiple_of(me * cols + h * hc, hc), hc), :]
    loads[2].wait()
    skew(staps_ref, padded, False, rows, band_s)

    groups2 = sources // GROUP
    per2 = GROUP // rows
    own2 = me // per2
    lane = lax.broadcasted_iota(jnp.int32, (hc, 2 * rows), 1)
    for h in range(halves):
        drain(foc_in.at[h, pl.ds(0, panels - 1)], recv1.at[h])
        for j in range(panels):
            x = foc_in[h, j]
            at = 2 * rows * j
            w2[0:hc, at : at + 2 * rows] = jnp.where(lane < rows, x, -x)
            w2[hc : 2 * hc, at : at + 2 * rows] = jnp.concatenate([x[:, rows:], x[:, :rows]], axis=1)

        @pl.loop(0, groups2)
        def _(n):
            g = order(n, own2, groups2, INNER2, CROSS2)
            first = pl.multiple_of(g * GROUP, GROUP)
            lhs = jnp.concatenate(
                [
                    band_s[pl.ds(pl.multiple_of(sources - rows * (jb + 1) + first, rows), GROUP), :]
                    for jb in range(panels)
                ],
                axis=1,
            )
            out = lax.dot_general(lhs, w2[...], nt, preferred_element_type=jnp.float32)
            mul[h, pl.ds(first, GROUP), :] = out.astype(jnp.bfloat16)
            for d in range(per2):
                dest = g * per2 + d

                @pl.when(dest != me)
                def _():
                    copy2(h, dest, me).start()

        mul_in[h, me] = mul[h, pl.ds(pl.multiple_of(me * rows, rows), rows), :]

    def fold(v):
        return jnp.sum(v.reshape(rows // SUBLANES, SUBLANES, LANES), axis=0)

    near = LANES // cols
    chunks = per2 // near

    def gather(q, count, acc):
        if count:
            drain(mul_in.at[:, pl.ds(q * per2, count)], recv2.at[q])

        def step(n, acc):
            cb = q * chunks + n
            blocks = [mul_in[h, cb * near + d] for d in range(near) for h in range(halves)]
            mre = jnp.concatenate([b[:, :hc] for b in blocks], axis=1)
            mim = jnp.concatenate([b[:, hc:] for b in blocks], axis=1)
            at = pl.ds(pl.multiple_of(cb * LANES, LANES), LANES)
            mult_ref[0, 0, :, at] = mre
            mult_ref[0, 1, :, at] = mim
            mre = mre.astype(jnp.float32)
            mim = mim.astype(jnp.float32)
            pre = rec_ref[0, 0, :, at]
            pim = rec_ref[0, 1, :, at]
            return (
                acc[0] + fold(mre * pre + mim * pim),
                acc[1] + fold(mre * pim - mim * pre),
                acc[2] + fold(mre * mre + mim * mim),
            )

        return lax.fori_loop(0, chunks, step, acc)

    zero = jnp.zeros((SUBLANES, LANES), jnp.float32)
    wide = groups2 // planes
    place = own2 - plane * wide

    def visit(n, acc):
        m = n // wide
        p = jnp.where(plane < planes // 2, plane, planes - 1 - plane)
        q = jnp.where(m == 0, p, jnp.where(m < planes // 2, m - (m <= p), planes + planes // 2 - 1 - m))
        q = jnp.where(plane < planes // 2, q, planes - 1 - q)
        at = lax.rem(n, wide)
        return gather(q * wide + jnp.where(m == 0, lax.rem(place + at, wide), lax.rem(place + 1 + at, wide)), per2, acc)

    num_re, num_im, energy = lax.fori_loop(1, groups2, visit, gather(own2, per2 - 1, (zero, zero, zero)))
    sub = lax.broadcasted_iota(jnp.int32, (SUBLANES, LANES), 0)
    num_re, num_im, energy = (jnp.sum(v, axis=0, keepdims=True) for v in (num_re, num_im, energy))
    part = jnp.where(sub == 0, num_re, jnp.where(sub == 1, num_im, jnp.where(sub == 2, energy, 0.0)))
    sums[...] = part
    sums_in[me] = part

    @pl.loop(1, panels)
    def _(o):
        copy3(peer(o), me).start()

    drain(foc.at[pl.ds(0, width - cols), :], send1)
    drain(mul.at[:, pl.ds(0, sources - rows), :], send2)
    drain(sums_in.at[pl.ds(0, panels - 1)], recv3)
    drain(sums_in.at[pl.ds(0, panels - 1)], send3)

    total = jnp.sum(jnp.sum(sums_in[...], axis=0), axis=1, keepdims=True)
    fit = total[0:2, :] / (total[2:3, :] + 1e-06)
    fit_ref[...] = jnp.broadcast_to(
        jnp.concatenate([fit, jnp.zeros((6, 1), jnp.float32)], axis=0), (8, LANES)
    )


def subtract_kernel(rec_ref, mult_ref, fit_ref, prim_hbm, mult_hbm, prim, sem):
    mult_out = pltpu.make_async_copy(mult_ref, mult_hbm, sem.at[0])
    mult_out.start()
    fit_re = fit_ref[0:1, 0:1]
    fit_im = fit_ref[1:2, 0:1]
    rows = rec_ref.shape[2]
    strip = rows // STRIPS
    outs = []
    for i in range(STRIPS):
        at = slice(i * strip, (i + 1) * strip)
        mre = mult_ref[0, 0, at, :].astype(jnp.float32)
        mim = mult_ref[0, 1, at, :].astype(jnp.float32)
        prim[0, 0, at, :] = rec_ref[0, 0, at, :] - (fit_re * mre - fit_im * mim)
        prim[0, 1, at, :] = rec_ref[0, 1, at, :] - (fit_re * mim + fit_im * mre)
        out = pltpu.make_async_copy(prim.at[:, :, at, :], prim_hbm.at[:, :, at, :], sem.at[i + 1])
        out.start()
        outs.append(out)
    for out in outs:
        out.wait()
    mult_out.wait()


def per_device(recorded, receiver_kernel, source_kernel):
    rows, width = recorded.shape[2], recorded.shape[3]
    panels = lax.axis_size("panel")
    sources = rows * panels
    cols = width // panels
    bf16 = jnp.bfloat16
    vmem = pl.BlockSpec(memory_space=pltpu.VMEM)
    hc = min(cols, LANES // 2)
    halves = cols // hc
    planes = PLANES if (width // GROUP) % PLANES == 0 and (sources // GROUP) % PLANES == 0 else 1
    sem = pltpu.SemaphoreType.DMA
    hbm = pl.BlockSpec(memory_space=pltpu.HBM)
    rec, mult, fit = pl.pallas_call(
        functools.partial(exchange_kernel, panels, planes),
        out_shape=(
            jax.ShapeDtypeStruct(recorded.shape, jnp.float32),
            jax.ShapeDtypeStruct(recorded.shape, bf16),
            jax.ShapeDtypeStruct((8, LANES), jnp.float32),
        ),
        in_specs=[hbm] * 3,
        out_specs=(vmem, vmem, vmem),
        scratch_shapes=[
            pltpu.VMEM(receiver_kernel.shape, bf16),
            pltpu.VMEM(source_kernel.shape, bf16),
            sem((3,)),
            pltpu.VMEM((2, 2 * width), jnp.float32),
            pltpu.VMEM((2 * width, 2 * LANES), bf16),
            pltpu.VMEM((2 * sources, 2 * rows), bf16),
            pltpu.VMEM((2 * rows, width), bf16),
            pltpu.VMEM((2 * hc, 2 * sources), bf16),
            pltpu.VMEM((width, 2 * rows), bf16),
            pltpu.VMEM((halves, panels, hc, 2 * rows), bf16),
            pltpu.VMEM((halves, sources, 2 * hc), bf16),
            pltpu.VMEM((halves, panels, rows, 2 * hc), bf16),
            pltpu.VMEM((8, LANES), jnp.float32),
            pltpu.VMEM((panels, 8, LANES), jnp.float32),
            sem,
            sem((halves,)),
            sem,
            sem((sources // GROUP,)),
            sem,
            sem,
            pltpu.SemaphoreType.REGULAR((4,)),
        ],
        compiler_params=pltpu.CompilerParams(collective_id=0, has_side_effects=True, vmem_limit_bytes=50 * 2**20),
        name="exchange",
    )(
        *(pltpu.with_memory_space_constraint(x, pltpu.HBM) for x in (recorded, receiver_kernel, source_kernel))
    )
    return pl.pallas_call(
        subtract_kernel,
        out_shape=(
            jax.ShapeDtypeStruct(recorded.shape, jnp.float32),
            jax.ShapeDtypeStruct(recorded.shape, bf16),
        ),
        in_specs=[vmem] * 3,
        out_specs=(hbm, hbm),
        scratch_shapes=[pltpu.VMEM(recorded.shape, jnp.float32), pltpu.SemaphoreType.DMA((STRIPS + 1,))],
        compiler_params=pltpu.CompilerParams(vmem_limit_bytes=12 * 2**20),
        name="subtract",
    )(rec, mult, fit)


def solution(mesh):
    placed = (P("freq", None, "panel", None), P("freq", None, None), P("freq", None, None))
    return jax.shard_map(
        per_device,
        mesh=mesh,
        in_specs=placed,
        out_specs=(P("freq", None, "panel", None), P("freq", None, "panel", None)),
        check_vma=False,
    )
```

```python
import functools

import jax
import jax.numpy as jnp
from jax import lax
from jax.experimental import pallas as pl
from jax.experimental.pallas import tpu as pltpu
from jax.sharding import PartitionSpec as P

MESH = pl.DeviceIdType.MESH
LANES = 128
GROUP = 256
STRIP = 16
SUBLANES = 8
STRIPS = 4
PLANES = 4
INNER1 = True
CROSS1 = 0
INNER2 = False
CROSS2 = 1


def spread(taps_ref, padded, comp, flipped):
    length = padded.shape[1]
    rows = [padded[comp : comp + 1, at : at + LANES] for at in range(0, length, LANES)]
    if not flipped:
        return jnp.broadcast_to(jnp.concatenate(rows, axis=1), (STRIP, length))
    i = lax.broadcasted_iota(jnp.int32, (LANES, LANES), 0)
    j = lax.broadcasted_iota(jnp.int32, (LANES, LANES), 1)
    swap = jnp.where(i + j == LANES - 1, 1.0, 0.0).astype(jnp.bfloat16)
    tall = jnp.concatenate([jnp.broadcast_to(r, (SUBLANES, LANES)) for r in rows[::-1]], axis=0)
    tall = jnp.dot(tall.astype(jnp.bfloat16), swap, preferred_element_type=jnp.float32)
    x = jnp.concatenate([tall[at : at + SUBLANES] for at in range(0, tall.shape[0], SUBLANES)], axis=1)
    return jnp.concatenate([x] * (STRIP // SUBLANES), axis=0)


def skew(taps_ref, padded, flipped, block, band_ref):
    length = padded.shape[1]
    padded[...] = jnp.zeros_like(padded)
    padded[:, 0 : length - 1] = taps_ref[0].astype(jnp.float32)
    row = lax.broadcasted_iota(jnp.int32, (STRIP, length), 0)
    for comp in range(2):
        x = spread(taps_ref, padded, comp, flipped)
        x = pltpu.roll(x, 0, 1, stride=1, stride_axis=0)
        lane0 = comp * block
        xb = x.astype(jnp.bfloat16)
        for s in range(0, LANES, STRIP):
            shift = (s - (LANES - block) + (0 if flipped else 1)) % length
            y = jnp.concatenate([xb[:, length - shift :], xb[:, : length - shift]], axis=1) if shift else xb
            for m in range(length // LANES):
                at = length - LANES * (m + 1)
                band_ref[m * LANES + s : m * LANES + s + STRIP, lane0 : lane0 + block] = y[:, at : at + block]


def exchange_kernel(
    panels,
    planes,
    rec_hbm,
    rtaps_hbm,
    staps_hbm,
    rec_ref,
    mult_ref,
    fit_ref,
    rtaps_ref,
    staps_ref,
    load_sem,
    padded,
    band_r,
    band_s,
    w1,
    w2,
    foc,
    foc_in,
    mul,
    mul_in,
    sums,
    sums_in,
    send1,
    recv1,
    send2,
    recv2,
    send3,
    recv3,
    relay,
):
    me = lax.axis_index("panel")
    rows, width = rec_ref.shape[2], rec_ref.shape[3]
    sources = rows * panels
    cols = width // panels
    halves, hc = foc_in.shape[0], foc_in.shape[2]
    nt = (((1,), (1,)), ((), ()))
    side = panels // planes
    plane = me // side

    def order(n, own, groups, inner_first, cross):
        wide = groups // planes
        high = own // wide >= planes // 2
        m = n // wide
        if inner_first:
            q = jnp.where(m < planes // 2, planes // 2 + m, planes - 1 - m)
        else:
            q = jnp.where(m < planes // 2, planes - 1 - m, m - planes // 2)
        q = jnp.where(high, planes - 1 - q, q)
        return q * wide + lax.rem(lax.rem(own, wide) + cross + n, wide)

    def peer(o):
        return lax.rem(me + o, panels)

    loads = [
        pltpu.make_async_copy(src, dst, load_sem.at[i])
        for i, (src, dst) in enumerate(
            ((rtaps_hbm, rtaps_ref), (rec_hbm, rec_ref), (staps_hbm, staps_ref))
        )
    ]
    for load in loads[:2]:
        load.start()

    barrier = pltpu.get_barrier_semaphore()

    above = (plane > 0).astype(jnp.int32)
    below = (plane < planes - 1).astype(jnp.int32)
    groups1 = width // GROUP
    per1 = GROUP // cols
    own1 = me // per1
    wide1 = groups1 // planes

    def greet(o):
        pl.semaphore_signal(barrier, inc=1, device_id={"panel": o}, device_id_type=MESH)

    for d in range(per1):

        @pl.when(plane > 0)
        def _():
            greet(own1 * per1 - side + d)

        @pl.when(plane < planes - 1)
        def _():
            greet(own1 * per1 + side + d)

    @pl.loop(1, side)
    def _(o):
        greet(plane * side + lax.rem(me - plane * side + o, side))


    outer = jnp.logical_or(plane == 0, plane == planes - 1)
    inner = jnp.logical_not(outer)
    outward = jnp.where(plane * 2 < planes, -side, side)
    inward = -outward

    def tell(slot, step):
        pl.semaphore_signal(relay.at[slot], inc=1, device_id={"panel": me + step}, device_id_type=MESH)

    loads[0].wait()
    skew(rtaps_ref, padded, True, LANES, band_r)
    loads[2].start()
    loads[1].wait()
    for comp in range(2):
        w1[comp * rows : (comp + 1) * rows, :] = rec_ref[0, comp].astype(jnp.bfloat16)

    pl.semaphore_wait(barrier, side - 1 + per1 * (above + below))
    for k in range(1, wide1):
        dest = plane * side + lax.rem(me - plane * side + k * per1, side)
        pl.semaphore_signal(relay.at[3], inc=1, device_id={"panel": dest}, device_id_type=MESH)

    def copy1(h, dest, src):
        return pltpu.make_async_remote_copy(
            src_ref=foc.at[pl.ds(pl.multiple_of(dest * cols + h * hc, hc), hc), :],
            dst_ref=foc_in.at[h, src],
            send_sem=send1,
            recv_sem=recv1.at[h],
            device_id={"panel": dest},
            device_id_type=MESH,
        )

    def copy2(h, dest, src):
        return pltpu.make_async_remote_copy(
            src_ref=mul.at[h, pl.ds(pl.multiple_of(dest * rows, rows), rows), :],
            dst_ref=mul_in.at[h, src],
            send_sem=send2,
            recv_sem=recv2.at[src // per2],
            device_id={"panel": dest},
            device_id_type=MESH,
        )

    def drain(ref, sem):
        pltpu.make_async_copy(ref, ref, sem).wait()

    def copy3(dest, src):
        return pltpu.make_async_remote_copy(
            src_ref=sums,
            dst_ref=sums_in.at[src],
            send_sem=send3,
            recv_sem=recv3,
            device_id={"panel": dest},
            device_id_type=MESH,
        )

    @pl.loop(0, groups1)
    def _(n):
        g = order(n, own1, groups1, INNER1, CROSS1)
        if planes > 1:

            @pl.when(jnp.logical_and(inner, n == groups1 // planes))
            def _():
                pl.semaphore_wait(relay.at[0], 1)
                tell(2, outward)

        first = pl.multiple_of(g * GROUP, GROUP)
        parts = []
        for comp in range(2):
            lhs = jnp.concatenate(
                [
                    band_r[
                        pl.ds(pl.multiple_of(width - LANES * (kb + 1) + first, LANES), GROUP),
                        comp * LANES : (comp + 1) * LANES,
                    ]
                    for kb in range(width // LANES)
                ],
                axis=1,
            )
            parts.append(lax.dot_general(lhs, w1[...], nt, preferred_element_type=jnp.float32))
        re, im = parts
        out = jnp.concatenate([re[:, :rows] - im[:, rows:], re[:, rows:] + im[:, :rows]], axis=1)
        foc[pl.ds(first, GROUP), :] = out.astype(jnp.bfloat16)
        if planes > 1:

            @pl.when(jnp.logical_and(outer, n == 0))
            def _():
                pl.semaphore_wait(relay.at[1], 1)

            @pl.when(jnp.logical_and(outer, n == groups1 // planes))
            def _():
                pl.semaphore_wait(relay.at[2], 1)

        for d in range(per1):
            dest = g * per1 + d

            @pl.when(dest != me)
            def _():
                copy1(0, dest, me).start()

        @pl.when(n == 0)
        def _():
            if wide1 > 1:
                pl.semaphore_wait(relay.at[3], wide1 - 1)
            if planes > 1:

                @pl.when(inner)
                def _():
                    tell(0, inward)
                    tell(1, outward)

    for h in range(1, halves):

        @pl.loop(0, groups1)
        def _(n):
            for d in range(per1):
                dest = order(n, own1, groups1, INNER1, CROSS1) * per1 + d

                @pl.when(dest != me)
                def _():
                    copy1(h, dest, me).start()

    for h in range(halves):
        foc_in[h, me] = foc[pl.ds(pl.multiple_of(me * cols + h * hc, hc), hc), :]
    loads[2].wait()
    skew(staps_ref, padded, False, rows, band_s)

    groups2 = sources // GROUP
    per2 = GROUP // rows
    own2 = me // per2
    lane = lax.broadcasted_iota(jnp.int32, (hc, 2 * rows), 1)
    for h in range(halves):
        drain(foc_in.at[h, pl.ds(0, panels - 1)], recv1.at[h])
        for j in range(panels):
            x = foc_in[h, j]
            at = 2 * rows * j
            w2[0:hc, at : at + 2 * rows] = jnp.where(lane < rows, x, -x)
            w2[hc : 2 * hc, at : at + 2 * rows] = jnp.concatenate([x[:, rows:], x[:, :rows]], axis=1)

        @pl.loop(0, groups2)
        def _(n):
            g = order(n, own2, groups2, INNER2, CROSS2)
            first = pl.multiple_of(g * GROUP, GROUP)
            lhs = jnp.concatenate(
                [
                    band_s[pl.ds(pl.multiple_of(sources - rows * (jb + 1) + first, rows), GROUP), :]
                    for jb in range(panels)
                ],
                axis=1,
            )
            out = lax.dot_general(lhs, w2[...], nt, preferred_element_type=jnp.float32)
            mul[h, pl.ds(first, GROUP), :] = out.astype(jnp.bfloat16)
            for d in range(per2):
                dest = g * per2 + d

                @pl.when(dest != me)
                def _():
                    copy2(h, dest, me).start()

        mul_in[h, me] = mul[h, pl.ds(pl.multiple_of(me * rows, rows), rows), :]

    def fold(v):
        return jnp.sum(v.reshape(rows // SUBLANES, SUBLANES, LANES), axis=0)

    near = LANES // cols
    chunks = per2 // near

    def gather(q, count, acc):
        if count:
            drain(mul_in.at[:, pl.ds(q * per2, count)], recv2.at[q])

        def step(n, acc):
            cb = q * chunks + n
            blocks = [mul_in[h, cb * near + d] for d in range(near) for h in range(halves)]
            mre = jnp.concatenate([b[:, :hc] for b in blocks], axis=1)
            mim = jnp.concatenate([b[:, hc:] for b in blocks], axis=1)
            at = pl.ds(pl.multiple_of(cb * LANES, LANES), LANES)
            mult_ref[0, 0, :, at] = mre
            mult_ref[0, 1, :, at] = mim
            mre = mre.astype(jnp.float32)
            mim = mim.astype(jnp.float32)
            pre = rec_ref[0, 0, :, at]
            pim = rec_ref[0, 1, :, at]
            return (
                acc[0] + fold(mre * pre + mim * pim),
                acc[1] + fold(mre * pim - mim * pre),
                acc[2] + fold(mre * mre + mim * mim),
            )

        return lax.fori_loop(0, chunks, step, acc)

    zero = jnp.zeros((SUBLANES, LANES), jnp.float32)
    wide = groups2 // planes
    place = own2 - plane * wide

    def visit(n, acc):
        m = n // wide
        p = jnp.where(plane < planes // 2, plane, planes - 1 - plane)
        q = jnp.where(m == 0, p, jnp.where(m < planes // 2, m - (m <= p), planes + planes // 2 - 1 - m))
        q = jnp.where(plane < planes // 2, q, planes - 1 - q)
        at = lax.rem(n, wide)
        return gather(q * wide + jnp.where(m == 0, lax.rem(place + at, wide), lax.rem(place + 1 + at, wide)), per2, acc)

    num_re, num_im, energy = lax.fori_loop(1, groups2, visit, gather(own2, per2 - 1, (zero, zero, zero)))
    sub = lax.broadcasted_iota(jnp.int32, (SUBLANES, LANES), 0)
    num_re, num_im, energy = (jnp.sum(v, axis=0, keepdims=True) for v in (num_re, num_im, energy))
    part = jnp.where(sub == 0, num_re, jnp.where(sub == 1, num_im, jnp.where(sub == 2, energy, 0.0)))
    sums[...] = part
    sums_in[me] = part

    @pl.loop(0, panels)
    def _(o):
        @pl.when(o != me)
        def _():
            copy3(o, me).start()

    drain(foc.at[pl.ds(0, width - cols), :], send1)
    drain(mul.at[:, pl.ds(0, sources - rows), :], send2)
    drain(sums_in.at[pl.ds(0, panels - 1)], recv3)
    drain(sums_in.at[pl.ds(0, panels - 1)], send3)

    fit_ref[...] = jnp.sum(sums_in[...], axis=0)


def subtract_kernel(rec_ref, mult_ref, fit_ref, prim_hbm, mult_hbm, prim, sem):
    mult_out = pltpu.make_async_copy(mult_ref, mult_hbm, sem.at[0])
    mult_out.start()
    total = jnp.sum(fit_ref[...], axis=1, keepdims=True)
    fit_re = total[0:1, :] / (total[2:3, :] + 1e-06)
    fit_im = total[1:2, :] / (total[2:3, :] + 1e-06)
    rows = rec_ref.shape[2]
    strip = rows // STRIPS
    outs = []
    for i in range(STRIPS):
        at = slice(i * strip, (i + 1) * strip)
        mre = mult_ref[0, 0, at, :].astype(jnp.float32)
        mim = mult_ref[0, 1, at, :].astype(jnp.float32)
        prim[0, 0, at, :] = rec_ref[0, 0, at, :] - (fit_re * mre - fit_im * mim)
        prim[0, 1, at, :] = rec_ref[0, 1, at, :] - (fit_re * mim + fit_im * mre)
        out = pltpu.make_async_copy(prim.at[:, :, at, :], prim_hbm.at[:, :, at, :], sem.at[i + 1])
        out.start()
        outs.append(out)
    for out in outs:
        out.wait()
    mult_out.wait()


def per_device(recorded, receiver_kernel, source_kernel):
    rows, width = recorded.shape[2], recorded.shape[3]
    panels = lax.axis_size("panel")
    sources = rows * panels
    cols = width // panels
    bf16 = jnp.bfloat16
    vmem = pl.BlockSpec(memory_space=pltpu.VMEM)
    hc = min(cols, LANES // 2)
    halves = cols // hc
    planes = PLANES if (width // GROUP) % PLANES == 0 and (sources // GROUP) % PLANES == 0 else 1
    sem = pltpu.SemaphoreType.DMA
    hbm = pl.BlockSpec(memory_space=pltpu.HBM)
    rec, mult, fit = pl.pallas_call(
        functools.partial(exchange_kernel, panels, planes),
        out_shape=(
            jax.ShapeDtypeStruct(recorded.shape, jnp.float32),
            jax.ShapeDtypeStruct(recorded.shape, bf16),
            jax.ShapeDtypeStruct((8, LANES), jnp.float32),
        ),
        in_specs=[hbm] * 3,
        out_specs=(vmem, vmem, vmem),
        scratch_shapes=[
            pltpu.VMEM(receiver_kernel.shape, bf16),
            pltpu.VMEM(source_kernel.shape, bf16),
            sem((3,)),
            pltpu.VMEM((2, 2 * width), jnp.float32),
            pltpu.VMEM((2 * width, 2 * LANES), bf16),
            pltpu.VMEM((2 * sources, 2 * rows), bf16),
            pltpu.VMEM((2 * rows, width), bf16),
            pltpu.VMEM((2 * hc, 2 * sources), bf16),
            pltpu.VMEM((width, 2 * rows), bf16),
            pltpu.VMEM((halves, panels, hc, 2 * rows), bf16),
            pltpu.VMEM((halves, sources, 2 * hc), bf16),
            pltpu.VMEM((halves, panels, rows, 2 * hc), bf16),
            pltpu.VMEM((8, LANES), jnp.float32),
            pltpu.VMEM((panels, 8, LANES), jnp.float32),
            sem,
            sem((halves,)),
            sem,
            sem((sources // GROUP,)),
            sem,
            sem,
            pltpu.SemaphoreType.REGULAR((4,)),
        ],
        compiler_params=pltpu.CompilerParams(collective_id=0, has_side_effects=True, vmem_limit_bytes=50 * 2**20),
        name="exchange",
    )(
        *(pltpu.with_memory_space_constraint(x, pltpu.HBM) for x in (recorded, receiver_kernel, source_kernel))
    )
    return pl.pallas_call(
        subtract_kernel,
        out_shape=(
            jax.ShapeDtypeStruct(recorded.shape, jnp.float32),
            jax.ShapeDtypeStruct(recorded.shape, bf16),
        ),
        in_specs=[vmem] * 3,
        out_specs=(hbm, hbm),
        scratch_shapes=[pltpu.VMEM(recorded.shape, jnp.float32), pltpu.SemaphoreType.DMA((STRIPS + 1,))],
        compiler_params=pltpu.CompilerParams(vmem_limit_bytes=12 * 2**20),
        name="subtract",
    )(rec, mult, fit)


def solution(mesh):
    placed = (P("freq", None, "panel", None), P("freq", None, None), P("freq", None, None))
    return jax.shard_map(
        per_device,
        mesh=mesh,
        in_specs=placed,
        out_specs=(P("freq", None, "panel", None), P("freq", None, "panel", None)),
        check_vma=False,
    )
```

```python
import functools

import jax
import jax.numpy as jnp
from jax import lax
from jax.experimental import pallas as pl
from jax.experimental.pallas import tpu as pltpu
from jax.sharding import PartitionSpec as P

MESH = pl.DeviceIdType.MESH
LANES = 128
GROUP = 256
STRIP = 16
SUBLANES = 8
STRIPS = 4
PLANES = 4
INNER1 = True
CROSS1 = 0
INNER2 = False
CROSS2 = 1


def spread(taps_ref, padded, comp, flipped):
    length = padded.shape[1]
    rows = [padded[comp : comp + 1, at : at + LANES] for at in range(0, length, LANES)]
    if not flipped:
        return jnp.broadcast_to(jnp.concatenate(rows, axis=1), (STRIP, length))
    i = lax.broadcasted_iota(jnp.int32, (LANES, LANES), 0)
    j = lax.broadcasted_iota(jnp.int32, (LANES, LANES), 1)
    swap = jnp.where(i + j == LANES - 1, 1.0, 0.0).astype(jnp.bfloat16)
    tall = jnp.concatenate([jnp.broadcast_to(r, (SUBLANES, LANES)) for r in rows[::-1]], axis=0)
    tall = jnp.dot(tall.astype(jnp.bfloat16), swap, preferred_element_type=jnp.float32)
    x = jnp.concatenate([tall[at : at + SUBLANES] for at in range(0, tall.shape[0], SUBLANES)], axis=1)
    return jnp.concatenate([x] * (STRIP // SUBLANES), axis=0)


def skew(taps_ref, padded, flipped, block, band_ref):
    length = padded.shape[1]
    padded[...] = jnp.zeros_like(padded)
    padded[:, 0 : length - 1] = taps_ref[0].astype(jnp.float32)
    row = lax.broadcasted_iota(jnp.int32, (STRIP, length), 0)
    for comp in range(2):
        x = spread(taps_ref, padded, comp, flipped)
        x = pltpu.roll(x, 0, 1, stride=1, stride_axis=0)
        lane0 = comp * block
        xb = x.astype(jnp.bfloat16)
        for s in range(0, LANES, STRIP):
            shift = (s - (LANES - block) + (0 if flipped else 1)) % length
            y = jnp.concatenate([xb[:, length - shift :], xb[:, : length - shift]], axis=1) if shift else xb
            for m in range(length // LANES):
                at = length - LANES * (m + 1)
                band_ref[m * LANES + s : m * LANES + s + STRIP, lane0 : lane0 + block] = y[:, at : at + block]


def exchange_kernel(
    panels,
    planes,
    rec_hbm,
    rtaps_hbm,
    staps_hbm,
    rec_ref,
    mult_ref,
    fit_ref,
    rtaps_ref,
    staps_ref,
    load_sem,
    padded,
    band_r,
    band_s,
    w1,
    w2,
    foc,
    foc_in,
    mul,
    mul_in,
    sums,
    sums_in,
    send1,
    recv1,
    send2,
    recv2,
    send3,
    recv3,
    relay,
):
    me = lax.axis_index("panel")
    rows, width = rec_ref.shape[2], rec_ref.shape[3]
    sources = rows * panels
    cols = width // panels
    halves, hc = foc_in.shape[0], foc_in.shape[2]
    nt = (((1,), (1,)), ((), ()))
    side = panels // planes
    plane = me // side

    def order(n, own, groups, inner_first, cross):
        wide = groups // planes
        high = own // wide >= planes // 2
        m = n // wide
        if inner_first:
            q = jnp.where(m < planes // 2, planes // 2 + m, planes - 1 - m)
        else:
            q = jnp.where(m < planes // 2, planes - 1 - m, m - planes // 2)
        q = jnp.where(high, planes - 1 - q, q)
        turn = jnp.where(m == planes // 2 - 1, cross, 0)
        return q * wide + lax.rem(lax.rem(own, wide) + turn + n, wide)

    def peer(o):
        return lax.rem(me + o, panels)

    loads = [
        pltpu.make_async_copy(src, dst, load_sem.at[i])
        for i, (src, dst) in enumerate(
            ((rtaps_hbm, rtaps_ref), (rec_hbm, rec_ref), (staps_hbm, staps_ref))
        )
    ]
    for load in loads[:2]:
        load.start()

    barrier = pltpu.get_barrier_semaphore()

    above = (plane > 0).astype(jnp.int32)
    below = (plane < planes - 1).astype(jnp.int32)
    groups1 = width // GROUP
    per1 = GROUP // cols
    own1 = me // per1
    wide1 = groups1 // planes

    def greet(o):
        pl.semaphore_signal(barrier, inc=1, device_id={"panel": o}, device_id_type=MESH)

    for d in range(per1):

        @pl.when(plane > 0)
        def _():
            greet(own1 * per1 - side + d)

        @pl.when(plane < planes - 1)
        def _():
            greet(own1 * per1 + side + d)

    @pl.loop(1, side)
    def _(o):
        greet(plane * side + lax.rem(me - plane * side + o, side))


    outer = jnp.logical_or(plane == 0, plane == planes - 1)
    inner = jnp.logical_not(outer)
    outward = jnp.where(plane * 2 < planes, -side, side)
    inward = -outward

    def tell(slot, step):
        pl.semaphore_signal(relay.at[slot], inc=1, device_id={"panel": me + step}, device_id_type=MESH)

    loads[0].wait()
    skew(rtaps_ref, padded, True, LANES, band_r)
    loads[2].start()
    loads[1].wait()
    for comp in range(2):
        w1[comp * rows : (comp + 1) * rows, :] = rec_ref[0, comp].astype(jnp.bfloat16)

    pl.semaphore_wait(barrier, side - 1 + per1 * (above + below))
    for k in range(1, wide1):
        dest = plane * side + lax.rem(me - plane * side + k * per1, side)
        pl.semaphore_signal(relay.at[3], inc=1, device_id={"panel": dest}, device_id_type=MESH)

    def copy1(h, dest, src):
        return pltpu.make_async_remote_copy(
            src_ref=foc.at[pl.ds(pl.multiple_of(dest * cols + h * hc, hc), hc), :],
            dst_ref=foc_in.at[h, src],
            send_sem=send1,
            recv_sem=recv1.at[h],
            device_id={"panel": dest},
            device_id_type=MESH,
        )

    def copy2(h, dest, src):
        return pltpu.make_async_remote_copy(
            src_ref=mul.at[h, pl.ds(pl.multiple_of(dest * rows, rows), rows), :],
            dst_ref=mul_in.at[h, src],
            send_sem=send2,
            recv_sem=recv2.at[src // per2],
            device_id={"panel": dest},
            device_id_type=MESH,
        )

    def drain(ref, sem):
        pltpu.make_async_copy(ref, ref, sem).wait()

    def copy3(dest, src):
        return pltpu.make_async_remote_copy(
            src_ref=sums,
            dst_ref=sums_in.at[src],
            send_sem=send3,
            recv_sem=recv3,
            device_id={"panel": dest},
            device_id_type=MESH,
        )

    @pl.loop(0, groups1)
    def _(n):
        g = order(n, own1, groups1, INNER1, CROSS1)
        if planes > 1:

            @pl.when(jnp.logical_and(inner, n == groups1 // planes))
            def _():
                pl.semaphore_wait(relay.at[0], 1)
                tell(2, outward)

        first = pl.multiple_of(g * GROUP, GROUP)
        parts = []
        for comp in range(2):
            lhs = jnp.concatenate(
                [
                    band_r[
                        pl.ds(pl.multiple_of(width - LANES * (kb + 1) + first, LANES), GROUP),
                        comp * LANES : (comp + 1) * LANES,
                    ]
                    for kb in range(width // LANES)
                ],
                axis=1,
            )
            parts.append(lax.dot_general(lhs, w1[...], nt, preferred_element_type=jnp.float32))
        re, im = parts
        out = jnp.concatenate([re[:, :rows] - im[:, rows:], re[:, rows:] + im[:, :rows]], axis=1)
        foc[pl.ds(first, GROUP), :] = out.astype(jnp.bfloat16)
        if planes > 1:

            @pl.when(jnp.logical_and(outer, n == 0))
            def _():
                pl.semaphore_wait(relay.at[1], 1)

            @pl.when(jnp.logical_and(outer, n == groups1 // planes))
            def _():
                pl.semaphore_wait(relay.at[2], 1)

        for d in range(per1):
            dest = g * per1 + d

            @pl.when(dest != me)
            def _():
                copy1(0, dest, me).start()

        @pl.when(n == 0)
        def _():
            if wide1 > 1:
                pl.semaphore_wait(relay.at[3], wide1 - 1)
            if planes > 1:

                @pl.when(inner)
                def _():
                    tell(0, inward)
                    tell(1, outward)

    for h in range(1, halves):

        @pl.loop(0, groups1)
        def _(n):
            for d in range(per1):
                dest = order(n, own1, groups1, INNER1, CROSS1) * per1 + d

                @pl.when(dest != me)
                def _():
                    copy1(h, dest, me).start()

    for h in range(halves):
        foc_in[h, me] = foc[pl.ds(pl.multiple_of(me * cols + h * hc, hc), hc), :]
    loads[2].wait()
    skew(staps_ref, padded, False, rows, band_s)

    groups2 = sources // GROUP
    per2 = GROUP // rows
    own2 = me // per2
    lane = lax.broadcasted_iota(jnp.int32, (hc, 2 * rows), 1)
    for h in range(halves):
        drain(foc_in.at[h, pl.ds(0, panels - 1)], recv1.at[h])
        for j in range(panels):
            x = foc_in[h, j]
            at = 2 * rows * j
            w2[0:hc, at : at + 2 * rows] = jnp.where(lane < rows, x, -x)
            w2[hc : 2 * hc, at : at + 2 * rows] = jnp.concatenate([x[:, rows:], x[:, :rows]], axis=1)

        @pl.loop(0, groups2)
        def _(n):
            g = order(n, own2, groups2, INNER2, CROSS2)
            first = pl.multiple_of(g * GROUP, GROUP)
            lhs = jnp.concatenate(
                [
                    band_s[pl.ds(pl.multiple_of(sources - rows * (jb + 1) + first, rows), GROUP), :]
                    for jb in range(panels)
                ],
                axis=1,
            )
            out = lax.dot_general(lhs, w2[...], nt, preferred_element_type=jnp.float32)
            mul[h, pl.ds(first, GROUP), :] = out.astype(jnp.bfloat16)
            for d in range(per2):
                dest = g * per2 + d

                @pl.when(dest != me)
                def _():
                    copy2(h, dest, me).start()

        mul_in[h, me] = mul[h, pl.ds(pl.multiple_of(me * rows, rows), rows), :]

    def fold(v):
        return jnp.sum(v.reshape(rows // SUBLANES, SUBLANES, LANES), axis=0)

    near = LANES // cols
    chunks = per2 // near

    def gather(q, count, acc):
        if count:
            drain(mul_in.at[:, pl.ds(q * per2, count)], recv2.at[q])

        def step(n, acc):
            cb = q * chunks + n
            blocks = [mul_in[h, cb * near + d] for d in range(near) for h in range(halves)]
            mre = jnp.concatenate([b[:, :hc] for b in blocks], axis=1)
            mim = jnp.concatenate([b[:, hc:] for b in blocks], axis=1)
            at = pl.ds(pl.multiple_of(cb * LANES, LANES), LANES)
            mult_ref[0, 0, :, at] = mre
            mult_ref[0, 1, :, at] = mim
            mre = mre.astype(jnp.float32)
            mim = mim.astype(jnp.float32)
            pre = rec_ref[0, 0, :, at]
            pim = rec_ref[0, 1, :, at]
            return (
                acc[0] + fold(mre * pre + mim * pim),
                acc[1] + fold(mre * pim - mim * pre),
                acc[2] + fold(mre * mre + mim * mim),
            )

        return lax.fori_loop(0, chunks, step, acc)

    zero = jnp.zeros((SUBLANES, LANES), jnp.float32)
    wide = groups2 // planes
    place = own2 - plane * wide

    def visit(n, acc):
        m = n // wide
        p = jnp.where(plane < planes // 2, plane, planes - 1 - plane)
        q = jnp.where(m == 0, p, jnp.where(m < planes // 2, m - (m <= p), planes + planes // 2 - 1 - m))
        q = jnp.where(plane < planes // 2, q, planes - 1 - q)
        at = lax.rem(n, wide)
        return gather(q * wide + jnp.where(m == 0, lax.rem(place + at, wide), lax.rem(place + 1 + at, wide)), per2, acc)

    num_re, num_im, energy = lax.fori_loop(1, groups2, visit, gather(own2, per2 - 1, (zero, zero, zero)))
    sub = lax.broadcasted_iota(jnp.int32, (SUBLANES, LANES), 0)
    num_re, num_im, energy = (jnp.sum(v, axis=0, keepdims=True) for v in (num_re, num_im, energy))
    part = jnp.where(sub == 0, num_re, jnp.where(sub == 1, num_im, jnp.where(sub == 2, energy, 0.0)))
    sums[...] = part
    sums_in[me] = part

    @pl.loop(0, panels)
    def _(o):
        @pl.when(o != me)
        def _():
            copy3(o, me).start()

    drain(foc.at[pl.ds(0, width - cols), :], send1)
    drain(mul.at[:, pl.ds(0, sources - rows), :], send2)
    drain(sums_in.at[pl.ds(0, panels - 1)], recv3)
    drain(sums_in.at[pl.ds(0, panels - 1)], send3)

    fit_ref[...] = jnp.sum(sums_in[...], axis=0)


def subtract_kernel(rec_ref, mult_ref, fit_ref, prim_hbm, mult_hbm, prim, sem):
    mult_out = pltpu.make_async_copy(mult_ref, mult_hbm, sem.at[0])
    mult_out.start()
    total = jnp.sum(fit_ref[...], axis=1, keepdims=True)
    fit_re = total[0:1, :] / (total[2:3, :] + 1e-06)
    fit_im = total[1:2, :] / (total[2:3, :] + 1e-06)
    rows = rec_ref.shape[2]
    strip = rows // STRIPS
    outs = []
    for i in range(STRIPS):
        at = slice(i * strip, (i + 1) * strip)
        mre = mult_ref[0, 0, at, :].astype(jnp.float32)
        mim = mult_ref[0, 1, at, :].astype(jnp.float32)
        prim[0, 0, at, :] = rec_ref[0, 0, at, :] - (fit_re * mre - fit_im * mim)
        prim[0, 1, at, :] = rec_ref[0, 1, at, :] - (fit_re * mim + fit_im * mre)
        out = pltpu.make_async_copy(prim.at[:, :, at, :], prim_hbm.at[:, :, at, :], sem.at[i + 1])
        out.start()
        outs.append(out)
    for out in outs:
        out.wait()
    mult_out.wait()


def per_device(recorded, receiver_kernel, source_kernel):
    rows, width = recorded.shape[2], recorded.shape[3]
    panels = lax.axis_size("panel")
    sources = rows * panels
    cols = width // panels
    bf16 = jnp.bfloat16
    vmem = pl.BlockSpec(memory_space=pltpu.VMEM)
    hc = min(cols, LANES // 2)
    halves = cols // hc
    planes = PLANES if (width // GROUP) % PLANES == 0 and (sources // GROUP) % PLANES == 0 else 1
    sem = pltpu.SemaphoreType.DMA
    hbm = pl.BlockSpec(memory_space=pltpu.HBM)
    rec, mult, fit = pl.pallas_call(
        functools.partial(exchange_kernel, panels, planes),
        out_shape=(
            jax.ShapeDtypeStruct(recorded.shape, jnp.float32),
            jax.ShapeDtypeStruct(recorded.shape, bf16),
            jax.ShapeDtypeStruct((8, LANES), jnp.float32),
        ),
        in_specs=[hbm] * 3,
        out_specs=(vmem, vmem, vmem),
        scratch_shapes=[
            pltpu.VMEM(receiver_kernel.shape, bf16),
            pltpu.VMEM(source_kernel.shape, bf16),
            sem((3,)),
            pltpu.VMEM((2, 2 * width), jnp.float32),
            pltpu.VMEM((2 * width, 2 * LANES), bf16),
            pltpu.VMEM((2 * sources, 2 * rows), bf16),
            pltpu.VMEM((2 * rows, width), bf16),
            pltpu.VMEM((2 * hc, 2 * sources), bf16),
            pltpu.VMEM((width, 2 * rows), bf16),
            pltpu.VMEM((halves, panels, hc, 2 * rows), bf16),
            pltpu.VMEM((halves, sources, 2 * hc), bf16),
            pltpu.VMEM((halves, panels, rows, 2 * hc), bf16),
            pltpu.VMEM((8, LANES), jnp.float32),
            pltpu.VMEM((panels, 8, LANES), jnp.float32),
            sem,
            sem((halves,)),
            sem,
            sem((sources // GROUP,)),
            sem,
            sem,
            pltpu.SemaphoreType.REGULAR((4,)),
        ],
        compiler_params=pltpu.CompilerParams(collective_id=0, has_side_effects=True, vmem_limit_bytes=50 * 2**20),
        name="exchange",
    )(
        *(pltpu.with_memory_space_constraint(x, pltpu.HBM) for x in (recorded, receiver_kernel, source_kernel))
    )
    return pl.pallas_call(
        subtract_kernel,
        out_shape=(
            jax.ShapeDtypeStruct(recorded.shape, jnp.float32),
            jax.ShapeDtypeStruct(recorded.shape, bf16),
        ),
        in_specs=[vmem] * 3,
        out_specs=(hbm, hbm),
        scratch_shapes=[pltpu.VMEM(recorded.shape, jnp.float32), pltpu.SemaphoreType.DMA((STRIPS + 1,))],
        compiler_params=pltpu.CompilerParams(vmem_limit_bytes=12 * 2**20),
        name="subtract",
    )(rec, mult, fit)


def solution(mesh):
    placed = (P("freq", None, "panel", None), P("freq", None, None), P("freq", None, None))
    return jax.shard_map(
        per_device,
        mesh=mesh,
        in_specs=placed,
        out_specs=(P("freq", None, "panel", None), P("freq", None, "panel", None)),
        check_vma=False,
    )
```

```python
import functools

import jax
import jax.numpy as jnp
from jax import lax
from jax.experimental import pallas as pl
from jax.experimental.pallas import tpu as pltpu
from jax.sharding import PartitionSpec as P

MESH = pl.DeviceIdType.MESH
LANES = 128
GROUP = 256
STRIP = 16
SUBLANES = 8
STRIPS = 4
PLANES = 4
INNER1 = True
CROSS1 = 0
INNER2 = False
CROSS2 = 1


def spread(taps_ref, padded, comp, flipped):
    length = padded.shape[1]
    rows = [padded[comp : comp + 1, at : at + LANES] for at in range(0, length, LANES)]
    if not flipped:
        return jnp.broadcast_to(jnp.concatenate(rows, axis=1), (STRIP, length))
    i = lax.broadcasted_iota(jnp.int32, (LANES, LANES), 0)
    j = lax.broadcasted_iota(jnp.int32, (LANES, LANES), 1)
    swap = jnp.where(i + j == LANES - 1, 1.0, 0.0).astype(jnp.bfloat16)
    tall = jnp.concatenate([jnp.broadcast_to(r, (SUBLANES, LANES)) for r in rows[::-1]], axis=0)
    tall = jnp.dot(tall.astype(jnp.bfloat16), swap, preferred_element_type=jnp.float32)
    x = jnp.concatenate([tall[at : at + SUBLANES] for at in range(0, tall.shape[0], SUBLANES)], axis=1)
    return jnp.concatenate([x] * (STRIP // SUBLANES), axis=0)


def skew(taps_ref, padded, flipped, block, band_ref):
    length = padded.shape[1]
    padded[...] = jnp.zeros_like(padded)
    padded[:, 0 : length - 1] = taps_ref[0].astype(jnp.float32)
    row = lax.broadcasted_iota(jnp.int32, (STRIP, length), 0)
    for comp in range(2):
        x = spread(taps_ref, padded, comp, flipped)
        x = pltpu.roll(x, 0, 1, stride=1, stride_axis=0)
        lane0 = comp * block
        xb = x.astype(jnp.bfloat16)
        for s in range(0, LANES, STRIP):
            shift = (s - (LANES - block) + (0 if flipped else 1)) % length
            y = jnp.concatenate([xb[:, length - shift :], xb[:, : length - shift]], axis=1) if shift else xb
            for m in range(length // LANES):
                at = length - LANES * (m + 1)
                band_ref[m * LANES + s : m * LANES + s + STRIP, lane0 : lane0 + block] = y[:, at : at + block]


def exchange_kernel(
    panels,
    planes,
    rec_hbm,
    rtaps_hbm,
    staps_hbm,
    rec_ref,
    mult_ref,
    fit_ref,
    rtaps_ref,
    staps_ref,
    load_sem,
    padded,
    band_r,
    band_s,
    w1,
    w2,
    foc,
    foc_in,
    mul,
    mul_in,
    sums,
    sums_in,
    send1,
    recv1,
    send2,
    recv2,
    send3,
    recv3,
    relay,
):
    me = lax.axis_index("panel")
    rows, width = rec_ref.shape[2], rec_ref.shape[3]
    sources = rows * panels
    cols = width // panels
    halves, hc = foc_in.shape[0], foc_in.shape[2]
    nt = (((1,), (1,)), ((), ()))
    side = panels // planes
    plane = me // side

    def order(n, own, groups, inner_first, cross):
        wide = groups // planes
        high = own // wide >= planes // 2
        m = n // wide
        if inner_first:
            q = jnp.where(m < planes // 2, planes // 2 + m, planes - 1 - m)
        else:
            q = jnp.where(m < planes // 2, planes - 1 - m, m - planes // 2)
        q = jnp.where(high, planes - 1 - q, q)
        turn = jnp.where(m == planes // 2 - 1, cross, 0)
        return q * wide + lax.rem(lax.rem(own, wide) + turn + n, wide)

    def peer(o):
        return lax.rem(me + o, panels)

    loads = [
        pltpu.make_async_copy(src, dst, load_sem.at[i])
        for i, (src, dst) in enumerate(
            ((rtaps_hbm, rtaps_ref), (rec_hbm, rec_ref), (staps_hbm, staps_ref))
        )
    ]
    for load in loads[:2]:
        load.start()

    barrier = pltpu.get_barrier_semaphore()

    above = (plane > 0).astype(jnp.int32)
    below = (plane < planes - 1).astype(jnp.int32)
    groups1 = width // GROUP
    per1 = GROUP // cols
    own1 = me // per1
    wide1 = groups1 // planes

    def greet(o):
        pl.semaphore_signal(barrier, inc=1, device_id={"panel": o}, device_id_type=MESH)

    for d in range(per1):

        @pl.when(plane > 0)
        def _():
            greet(own1 * per1 - side + d)

        @pl.when(plane < planes - 1)
        def _():
            greet(own1 * per1 + side + d)

    @pl.loop(1, side)
    def _(o):
        greet(plane * side + lax.rem(me - plane * side + o, side))


    outer = jnp.logical_or(plane == 0, plane == planes - 1)
    inner = jnp.logical_not(outer)
    outward = jnp.where(plane * 2 < planes, -side, side)
    inward = -outward

    def tell(slot, step):
        pl.semaphore_signal(relay.at[slot], inc=1, device_id={"panel": me + step}, device_id_type=MESH)

    loads[0].wait()
    skew(rtaps_ref, padded, True, LANES, band_r)
    loads[2].start()
    loads[1].wait()
    for comp in range(2):
        w1[comp * rows : (comp + 1) * rows, :] = rec_ref[0, comp].astype(jnp.bfloat16)

    pl.semaphore_wait(barrier, side - 1 + per1 * (above + below))
    for k in range(1, wide1):
        dest = plane * side + lax.rem(me - plane * side + k * per1, side)
        pl.semaphore_signal(relay.at[3], inc=1, device_id={"panel": dest}, device_id_type=MESH)

    def copy1(h, dest, src):
        return pltpu.make_async_remote_copy(
            src_ref=foc.at[pl.ds(pl.multiple_of(dest * cols + h * hc, hc), hc), :],
            dst_ref=foc_in.at[h, src],
            send_sem=send1,
            recv_sem=recv1.at[h],
            device_id={"panel": dest},
            device_id_type=MESH,
        )

    def copy2(h, dest, src):
        return pltpu.make_async_remote_copy(
            src_ref=mul.at[h, pl.ds(pl.multiple_of(dest * rows, rows), rows), :],
            dst_ref=mul_in.at[h, src],
            send_sem=send2,
            recv_sem=recv2.at[src // per2],
            device_id={"panel": dest},
            device_id_type=MESH,
        )

    def drain(ref, sem):
        pltpu.make_async_copy(ref, ref, sem).wait()

    def copy3(dest, src):
        return pltpu.make_async_remote_copy(
            src_ref=sums,
            dst_ref=sums_in.at[src],
            send_sem=send3,
            recv_sem=recv3,
            device_id={"panel": dest},
            device_id_type=MESH,
        )

    @pl.loop(0, groups1)
    def _(n):
        g = order(n, own1, groups1, INNER1, CROSS1)
        if planes > 1:

            @pl.when(jnp.logical_and(inner, n == groups1 // planes))
            def _():
                pl.semaphore_wait(relay.at[0], 1)
                tell(2, outward)

        first = pl.multiple_of(g * GROUP, GROUP)
        parts = []
        for comp in range(2):
            lhs = jnp.concatenate(
                [
                    band_r[
                        pl.ds(pl.multiple_of(width - LANES * (kb + 1) + first, LANES), GROUP),
                        comp * LANES : (comp + 1) * LANES,
                    ]
                    for kb in range(width // LANES)
                ],
                axis=1,
            )
            parts.append(lax.dot_general(lhs, w1[...], nt, preferred_element_type=jnp.float32))
        re, im = parts
        out = jnp.concatenate([re[:, :rows] - im[:, rows:], re[:, rows:] + im[:, :rows]], axis=1)
        foc[pl.ds(first, GROUP), :] = out.astype(jnp.bfloat16)
        if planes > 1:

            @pl.when(jnp.logical_and(outer, n == 0))
            def _():
                pl.semaphore_wait(relay.at[1], 1)

            @pl.when(jnp.logical_and(outer, n == groups1 // planes))
            def _():
                pl.semaphore_wait(relay.at[2], 1)

        for d in range(per1):
            dest = g * per1 + d

            @pl.when(dest != me)
            def _():
                copy1(0, dest, me).start()

        @pl.when(n == 0)
        def _():
            if wide1 > 1:
                pl.semaphore_wait(relay.at[3], wide1 - 1)
            if planes > 1:

                @pl.when(inner)
                def _():
                    tell(0, inward)
                    tell(1, outward)

    for h in range(1, halves):

        @pl.loop(0, groups1)
        def _(n):
            for d in range(per1):
                dest = order(n, own1, groups1, INNER1, CROSS1) * per1 + d

                @pl.when(dest != me)
                def _():
                    copy1(h, dest, me).start()

    for h in range(halves):
        foc_in[h, me] = foc[pl.ds(pl.multiple_of(me * cols + h * hc, hc), hc), :]
    loads[2].wait()
    skew(staps_ref, padded, False, rows, band_s)

    groups2 = sources // GROUP
    per2 = GROUP // rows
    own2 = me // per2
    lane = lax.broadcasted_iota(jnp.int32, (hc, 2 * rows), 1)
    for h in range(halves):
        drain(foc_in.at[h, pl.ds(0, panels - 1)], recv1.at[h])
        for j in range(panels):
            x = foc_in[h, j]
            at = 2 * rows * j
            w2[0:hc, at : at + 2 * rows] = jnp.where(lane < rows, x, -x)
            w2[hc : 2 * hc, at : at + 2 * rows] = jnp.concatenate([x[:, rows:], x[:, :rows]], axis=1)

        @pl.loop(0, groups2)
        def _(n):
            g = order(n, own2, groups2, INNER2, CROSS2)
            first = pl.multiple_of(g * GROUP, GROUP)
            lhs = jnp.concatenate(
                [
                    band_s[pl.ds(pl.multiple_of(sources - rows * (jb + 1) + first, rows), GROUP), :]
                    for jb in range(panels)
                ],
                axis=1,
            )
            out = lax.dot_general(lhs, w2[...], nt, preferred_element_type=jnp.float32)
            mul[h, pl.ds(first, GROUP), :] = out.astype(jnp.bfloat16)
            for d in range(per2):
                dest = g * per2 + d

                @pl.when(dest != me)
                def _():
                    copy2(h, dest, me).start()

        mul_in[h, me] = mul[h, pl.ds(pl.multiple_of(me * rows, rows), rows), :]

    def fold(v):
        return jnp.sum(v.reshape(rows // SUBLANES, SUBLANES, LANES), axis=0)

    near = LANES // cols
    chunks = per2 // near

    def gather(q, count, acc):
        if count:
            drain(mul_in.at[:, pl.ds(q * per2, count)], recv2.at[q])

        def step(n, acc):
            cb = q * chunks + n
            blocks = [mul_in[h, cb * near + d] for d in range(near) for h in range(halves)]
            mre = jnp.concatenate([b[:, :hc] for b in blocks], axis=1)
            mim = jnp.concatenate([b[:, hc:] for b in blocks], axis=1)
            at = pl.ds(pl.multiple_of(cb * LANES, LANES), LANES)
            mult_ref[0, 0, :, at] = mre
            mult_ref[0, 1, :, at] = mim
            mre = mre.astype(jnp.float32)
            mim = mim.astype(jnp.float32)
            pre = rec_ref[0, 0, :, at]
            pim = rec_ref[0, 1, :, at]
            return (
                acc[0] + fold(mre * pre + mim * pim),
                acc[1] + fold(mre * pim - mim * pre),
                acc[2] + fold(mre * mre + mim * mim),
            )

        return lax.fori_loop(0, chunks, step, acc, unroll=True)

    zero = jnp.zeros((SUBLANES, LANES), jnp.float32)
    wide = groups2 // planes
    place = own2 - plane * wide

    def visit(n, acc):
        m = n // wide
        p = jnp.where(plane < planes // 2, plane, planes - 1 - plane)
        q = jnp.where(m == 0, p, jnp.where(m < planes // 2, m - (m <= p), planes + planes // 2 - 1 - m))
        q = jnp.where(plane < planes // 2, q, planes - 1 - q)
        at = lax.rem(n, wide)
        return gather(q * wide + jnp.where(m == 0, lax.rem(place + at, wide), lax.rem(place + 1 + at, wide)), per2, acc)

    num_re, num_im, energy = lax.fori_loop(1, groups2, visit, gather(own2, per2 - 1, (zero, zero, zero)))
    sub = lax.broadcasted_iota(jnp.int32, (SUBLANES, LANES), 0)
    num_re, num_im, energy = (jnp.sum(v, axis=0, keepdims=True) for v in (num_re, num_im, energy))
    part = jnp.where(sub == 0, num_re, jnp.where(sub == 1, num_im, jnp.where(sub == 2, energy, 0.0)))
    sums[...] = part
    sums_in[me] = part

    @pl.loop(0, panels)
    def _(o):
        @pl.when(o != me)
        def _():
            copy3(o, me).start()

    drain(foc.at[pl.ds(0, width - cols), :], send1)
    drain(mul.at[:, pl.ds(0, sources - rows), :], send2)
    drain(sums_in.at[pl.ds(0, panels - 1)], recv3)
    drain(sums_in.at[pl.ds(0, panels - 1)], send3)

    fit_ref[...] = jnp.sum(sums_in[...], axis=0)


def subtract_kernel(rec_ref, mult_ref, fit_ref, prim_hbm, mult_hbm, prim, sem):
    mult_out = pltpu.make_async_copy(mult_ref, mult_hbm, sem.at[0])
    mult_out.start()
    total = jnp.sum(fit_ref[...], axis=1, keepdims=True)
    fit_re = total[0:1, :] / (total[2:3, :] + 1e-06)
    fit_im = total[1:2, :] / (total[2:3, :] + 1e-06)
    rows = rec_ref.shape[2]
    strip = rows // STRIPS
    outs = []
    for i in range(STRIPS):
        at = slice(i * strip, (i + 1) * strip)
        mre = mult_ref[0, 0, at, :].astype(jnp.float32)
        mim = mult_ref[0, 1, at, :].astype(jnp.float32)
        prim[0, 0, at, :] = rec_ref[0, 0, at, :] - (fit_re * mre - fit_im * mim)
        prim[0, 1, at, :] = rec_ref[0, 1, at, :] - (fit_re * mim + fit_im * mre)
        out = pltpu.make_async_copy(prim.at[:, :, at, :], prim_hbm.at[:, :, at, :], sem.at[i + 1])
        out.start()
        outs.append(out)
    for out in outs:
        out.wait()
    mult_out.wait()


def per_device(recorded, receiver_kernel, source_kernel):
    rows, width = recorded.shape[2], recorded.shape[3]
    panels = lax.axis_size("panel")
    sources = rows * panels
    cols = width // panels
    bf16 = jnp.bfloat16
    vmem = pl.BlockSpec(memory_space=pltpu.VMEM)
    hc = min(cols, LANES // 2)
    halves = cols // hc
    planes = PLANES if (width // GROUP) % PLANES == 0 and (sources // GROUP) % PLANES == 0 else 1
    sem = pltpu.SemaphoreType.DMA
    hbm = pl.BlockSpec(memory_space=pltpu.HBM)
    rec, mult, fit = pl.pallas_call(
        functools.partial(exchange_kernel, panels, planes),
        out_shape=(
            jax.ShapeDtypeStruct(recorded.shape, jnp.float32),
            jax.ShapeDtypeStruct(recorded.shape, bf16),
            jax.ShapeDtypeStruct((8, LANES), jnp.float32),
        ),
        in_specs=[hbm] * 3,
        out_specs=(vmem, vmem, vmem),
        scratch_shapes=[
            pltpu.VMEM(receiver_kernel.shape, bf16),
            pltpu.VMEM(source_kernel.shape, bf16),
            sem((3,)),
            pltpu.VMEM((2, 2 * width), jnp.float32),
            pltpu.VMEM((2 * width, 2 * LANES), bf16),
            pltpu.VMEM((2 * sources, 2 * rows), bf16),
            pltpu.VMEM((2 * rows, width), bf16),
            pltpu.VMEM((2 * hc, 2 * sources), bf16),
            pltpu.VMEM((width, 2 * rows), bf16),
            pltpu.VMEM((halves, panels, hc, 2 * rows), bf16),
            pltpu.VMEM((halves, sources, 2 * hc), bf16),
            pltpu.VMEM((halves, panels, rows, 2 * hc), bf16),
            pltpu.VMEM((8, LANES), jnp.float32),
            pltpu.VMEM((panels, 8, LANES), jnp.float32),
            sem,
            sem((halves,)),
            sem,
            sem((sources // GROUP,)),
            sem,
            sem,
            pltpu.SemaphoreType.REGULAR((4,)),
        ],
        compiler_params=pltpu.CompilerParams(collective_id=0, has_side_effects=True, vmem_limit_bytes=50 * 2**20),
        name="exchange",
    )(
        *(pltpu.with_memory_space_constraint(x, pltpu.HBM) for x in (recorded, receiver_kernel, source_kernel))
    )
    return pl.pallas_call(
        subtract_kernel,
        out_shape=(
            jax.ShapeDtypeStruct(recorded.shape, jnp.float32),
            jax.ShapeDtypeStruct(recorded.shape, bf16),
        ),
        in_specs=[vmem] * 3,
        out_specs=(hbm, hbm),
        scratch_shapes=[pltpu.VMEM(recorded.shape, jnp.float32), pltpu.SemaphoreType.DMA((STRIPS + 1,))],
        compiler_params=pltpu.CompilerParams(vmem_limit_bytes=12 * 2**20),
        name="subtract",
    )(rec, mult, fit)


def solution(mesh):
    placed = (P("freq", None, "panel", None), P("freq", None, None), P("freq", None, None))
    return jax.shard_map(
        per_device,
        mesh=mesh,
        in_specs=placed,
        out_specs=(P("freq", None, "panel", None), P("freq", None, "panel", None)),
        check_vma=False,
    )
```
